256 devices in a mesh: role: 4 (over z_lo), dp: 16 (over z_hi, x, core), tp: 4 (over y).
Axes of the slice: x: 4, y: 4, z: 8 (z_hi: 2, z_lo: 4; z = z_hi * 4 + z_lo), core: 2. Of those that a mesh axis runs over, the one named last changes fastest.
Arguments:
- activations: bfloat16 [16384, 8192], P(('role', 'dp'), 'tp'), may hold values from -6 to 6
- cotangent: bfloat16 [16384, 14336], P(('role', 'dp'), 'tp'), may hold values from -6 to 6
- block_keep: int32 [64], P(('role', 'dp')), may hold values 0 or 1
- input_factor: float32 [64, 8192], P(('role', 'dp'), 'tp'), may hold values from -0.5 to 0.5
- input_mean: float32 [64, 8192], P(('role', 'dp'), 'tp'), may hold values from -6 to 6
- input_square: float32 [64, 8192], P(('role', 'dp'), 'tp'), may hold values from 0.5 to 4
- output_factor: float32 [64, 14336], P(('role', 'dp'), 'tp'), may hold values from -0.3125 to 0.3125
- output_mean: float32 [64, 14336], P(('role', 'dp'), 'tp'), may hold values from -6 to 6
- output_square: float32 [64, 14336], P(('role', 'dp'), 'tp'), may hold values from 0.5 to 4
- frozen_base_rows: bfloat16 [14336, 8192], P(('dp', 'tp')), may hold values from -0.0625 to 0.0625
- prompts: bfloat16 [1024, 8192], P(('role', 'dp', 'tp')), may hold values from -6 to 6
Outputs:
- updated_input: float32 [64, 8192], P(('role', 'dp'), 'tp')
- updated_output: float32 [64, 14336], P(('role', 'dp'), 'tp')
- mean_input: float32 [64, 8192], P(('role', 'dp'), 'tp')
- mean_output: float32 [64, 14336], P(('role', 'dp'), 'tp')
- square_input: float32 [64, 8192], P(('role', 'dp'), 'tp')
- square_output: float32 [64, 14336], P(('role', 'dp'), 'tp')
- merged_weight_rows: bfloat16 [14336, 8192], P(('dp', 'tp'))
- projected: bfloat16 [14336, 1024], P(('dp', 'tp'), 'role')
The draws below stay inside these ranges and needn't reach their ends.
All inputs are finite; a program needn't handle non-finite values. No bound on the sum of `block_keep` on one device may be relied on, other than what follows from the above.
Results may differ from the reference program's by a relative error of at most 0.006.
Values may be sent and summed in bfloat16 or wider, within the bound.
A program may use at most 64 MiB of HBM per device.

```python
import math
import jax
import jax.numpy as jnp
from jax import lax

D = 8192
FFW = 14336
RANK = 64
ROLLOUT_TOKENS = 256
TOKENS = 16384
BLOCKS = 64
PROMPTS = 1024


def touch_ends(result, key, low, high):
    dims = result.shape
    place = [jax.random.randint(jax.random.fold_in(key, axis), (), 0, dims[axis]) for axis in range(len(dims))]
    result = result.at[tuple(place)].set(low)
    longest = dims.index(max(dims))
    place[longest] = (place[longest] + 1) % dims[longest]
    return result.at[tuple(place)].set(high)


def shard_levels(own_key, shape, cuts, smallest, top_value):
    factor_of, own = 1.0, jax.random.fold_in(own_key, 6)
    for dim, shards_of in cuts:
        draws = jnp.exp(jax.random.uniform(jax.random.fold_in(own, dim), (shards_of,), jnp.float32, smallest / len(cuts), top_value / len(cuts)))
        factor_of = factor_of * jnp.repeat(draws, shape[dim] // shards_of).reshape([-1 if axis == dim else 1 for axis in range(len(shape))])
    return factor_of


def scatter_about(own_key, shape, spread, limit, shards=(), dtype=jnp.bfloat16):
    array = jax.random.normal(own_key, shape, jnp.float32) * spread
    if len(shards) > 0:
        array = shard_levels(own_key, shape, shards, -0.22, 0.18) * array
    return jnp.clip(array, min=-limit, max=limit).astype(dtype)


def setup_inputs(seed: int = 0) -> dict:
    key_of = jax.random.split(jax.random.key(seed), 12)
    return {
        "activations": scatter_about(key_of[0], (TOKENS, D), 1.0, 6.0, ((0, 64), (1, 4))),
        "cotangent": scatter_about(key_of[1], (TOKENS, FFW), 1.0, 6.0, ((0, 64), (1, 4))),
        "block_keep": touch_ends((jax.random.randint(key_of[2], (BLOCKS,), 0, 4) < 3).astype(jnp.int32), jax.random.fold_in(key_of[2], 1), 0, 1),
        "input_factor": scatter_about(key_of[3], (RANK, D), 0.035, 0.5, ((0, 64), (1, 4)), jnp.float32),
        "input_mean": scatter_about(key_of[4], (RANK, D), 1.0, 6.0, ((0, 64), (1, 4)), jnp.float32),
        "input_square": jnp.clip(jnp.exp(math.log(4.0) - 2.0794415 * jax.random.uniform(key_of[5], (RANK, D), jnp.float32) ** shard_levels(key_of[5], (RANK, D), ((0, 64), (1, 4)), -0.2, 0.2)), 0.5, 4.0),
        "output_factor": scatter_about(key_of[6], (RANK, FFW), 0.02, 0.3125, ((0, 64), (1, 4)), jnp.float32),
        "output_mean": scatter_about(key_of[7], (RANK, FFW), 1.0, 6.0, ((0, 64), (1, 4)), jnp.float32),
        "output_square": jnp.clip(jnp.exp(math.log(4.0) - 2.0794415 * jax.random.uniform(key_of[8], (RANK, FFW), jnp.float32) ** shard_levels(key_of[8], (RANK, FFW), ((0, 64), (1, 4)), -0.2, 0.2)), 0.5, 4.0),
        "frozen_base_rows": scatter_about(key_of[9], (FFW, D), D ** -0.5, 0.0625, ((0, 64),)),
        "prompts": scatter_about(key_of[10], (PROMPTS, D), 1.0, 6.0, ((0, 256),)),
    }


adapter_scale = 2.0
learn_rate = 0.004
beta_one = 0.9
beta_two = 0.95
epsilon = 1e-08
first_fix = 1.0 - 0.9 ** 20
second_fix = 1.0 - 0.95 ** 20

def adam_update(factor, moment, square, gradient):
    moment_new = beta_one * moment + (1.0 - beta_one) * gradient
    square_new = beta_two * square + (1.0 - beta_two) * gradient * gradient
    factor_new = factor - learn_rate * (moment_new / first_fix) / (jnp.sqrt(square_new / second_fix) + epsilon)
    return (factor_new, moment_new, square_new)

def masked(values, block_keep):
    blocks = block_keep.shape[0]
    reshaped_rows = values.reshape(blocks, values.shape[0] // blocks, values.shape[1])
    weighted = reshaped_rows * block_keep.astype(jnp.float32)[:, None, None]
    return weighted.reshape(values.shape).astype(jnp.bfloat16)

def contract_rows(left, right):
    return lax.dot_general(left, right, (((0,), (0,)), ((), ())), preferred_element_type=jnp.float32)

def contract_cols(left, right):
    return lax.dot_general(left, right, (((1,), (1,)), ((), ())), preferred_element_type=jnp.float32)

def reference(activations, cotangent, block_keep, input_factor, input_mean, input_square, output_factor, output_mean, output_square, frozen_base_rows, prompts):
    input_rows = input_factor.astype(jnp.bfloat16)
    output_rows = output_factor.astype(jnp.bfloat16)
    low_input = jnp.dot(activations, input_rows.T, preferred_element_type=jnp.float32)
    low_grad = jnp.dot(cotangent, output_rows.T, preferred_element_type=jnp.float32)
    input_kept = masked(low_input, block_keep)
    grad_kept = masked(low_grad, block_keep)
    adapter_factor_scale = adapter_scale / ROLLOUT_TOKENS
    input_grad = contract_rows(grad_kept, activations) * adapter_factor_scale
    output_grad = contract_rows(input_kept, cotangent) * adapter_factor_scale
    input_new, input_moment, input_second = adam_update(input_factor, input_mean, input_square, input_grad)
    output_new, output_moment, output_second = adam_update(output_factor, output_mean, output_square, output_grad)
    adapter_delta_rows = contract_rows(output_new.astype(jnp.bfloat16), input_new.astype(jnp.bfloat16))
    merged_weight_rows = (frozen_base_rows.astype(jnp.float32) + adapter_scale * adapter_delta_rows).astype(jnp.bfloat16)
    projected = contract_cols(merged_weight_rows, prompts).astype(jnp.bfloat16)
    return (input_new, output_new, input_moment, output_moment, input_second, output_second, merged_weight_rows, projected)
```

```python
import jax
import jax.numpy as jnp
from jax import lax
from jax.experimental import pallas as pl
from jax.experimental.pallas import tpu as pltpu
from jax.sharding import PartitionSpec as P

ROLLOUT_TOKENS = 256
RANK = 64
LANES = 128
ROWS_A, ROWS_B = 16, 28
ROWS = ROWS_A + ROWS_B
NX, NY, NZ, NC = 4, 4, 8, 2
BLOCK = 224
WIDE = 256

adapter_scale = 2.0
learn_rate = 0.004
beta_one = 0.9
beta_two = 0.95
epsilon = 1e-08
first_fix = 1.0 - 0.9**20
second_fix = 1.0 - 0.95**20

F32, BF16 = jnp.float32, jnp.bfloat16
MESH = pl.DeviceIdType.MESH


def adam_update(factor, moment, square, gradient):
    moment_new = beta_one * moment + (1.0 - beta_one) * gradient
    square_new = beta_two * square + (1.0 - beta_two) * gradient * gradient
    factor_new = factor - learn_rate * (moment_new / first_fix) / (
        jnp.sqrt(square_new / second_fix) + epsilon
    )
    return (factor_new, moment_new, square_new)


def dot_nn(a, b):
    return lax.dot_general(a, b, (((1,), (0,)), ((), ())), preferred_element_type=F32)


def dot_nt(a, b):
    return lax.dot_general(a, b, (((1,), (1,)), ((), ())), preferred_element_type=F32)


def in_wide_blocks(rows):
    lane = lax.broadcasted_iota(jnp.int32, (1, LANES), 1)
    rolled = {0: rows}
    for off in (32, 64, 96):
        rolled[off] = pltpu.roll(rows, LANES - off, 1)
    out = []
    for k in range(16):
        row, off = divmod(BLOCK * k, LANES)
        turned = rolled[off]
        for half in range(2):
            first = turned[row + half : row + half + 1]
            if off == 0:
                out.append(first)
                continue
            last = min(row + half + 1, ROWS_B - 1)
            second = turned[last : last + 1]
            out.append(jnp.where(lane < LANES - off, first, second))
    return out


def exchange_kernel(
    act_hbm,
    cot_hbm,
    keep_ref,
    fa,
    ma,
    va,
    fb,
    mb,
    vb,
    prompts_hbm,
    grad_out,
    ha,
    bb,
    q,
    act,
    cot,
    g,
    stg8,
    w,
    low,
    stg64,
    p_send,
    r1,
    s2,
    r2,
    t32,
    t16,
    r3,
    ea,
    stga,
    ebz,
    ebx,
    ebd,
    stgb,
    bs,
    pr,
    pf,
    loc,
    ssem,
    rsem,
):
    z_lo = lax.axis_index("role")
    dp = lax.axis_index("dp")
    y = lax.axis_index("tp")
    c = lax.rem(dp, 2)
    x = lax.rem(lax.div(dp, 2), 4)
    zh = lax.div(dp, 8)
    z = zh * 4 + z_lo

    def at(x_=x, y_=y, z_=z, c_=c):
        return {
            "role": lax.rem(z_, 4),
            "dp": lax.div(z_, 4) * 8 + x_ * 2 + c_,
            "tp": y_,
        }

    def step(v, d, n):
        return lax.rem(v + d, n)

    other = 1 - c
    sibling = at(c_=other)
    xs = [step(x, d, NX) for d in range(NX)]
    ys = [step(y, d, NY) for d in range(NY)]
    zs = [step(z, d, NZ) for d in range(NZ)]
    from_x = [step(x, NX - d, NX) for d in range(NX)]
    from_y = [step(y, NY - d, NY) for d in range(NY)]
    from_z = [step(z, NZ - d, NZ) for d in range(NZ)]

    names = {}

    def copy(src, dst, key, device):
        i = names.setdefault(key, len(names))
        return pltpu.make_async_remote_copy(
            src_ref=src,
            dst_ref=dst,
            send_sem=ssem.at[i],
            recv_sem=rsem.at[i],
            device_id=device,
            device_id_type=MESH,
        )

    sent = []

    def send(src, dst, key, device):
        one = copy(src, dst, key, device)
        one.start()
        sent.append(one)

    def arrived(dst, key):
        copy(dst, dst, key, sibling).wait_recv()

    load_act = pltpu.make_async_copy(act_hbm, act, loc.at[0])
    load_cot = pltpu.make_async_copy(cot_hbm, cot, loc.at[1])
    load_act.start()
    load_cot.start()
    quarter = 2048

    def columns(yy):
        return prompts_hbm.at[:, pl.ds(pl.multiple_of(yy * quarter, quarter), quarter)]

    load_own = pltpu.make_async_copy(columns(y), pr.at[y], loc.at[2])
    load_own.start()

    barrier = pltpu.get_barrier_semaphore()
    peers = (
        [sibling]
        + [at(x_=v) for v in xs[1:]]
        + [at(y_=v) for v in ys[1:]]
        + [at(z_=v) for v in zs[1:]]
    )
    for peer in peers:
        pl.semaphore_signal(barrier, inc=1, device_id=peer, device_id_type=MESH)

    g[c, x, z, 0:ROWS_A, :] = fa[...].astype(BF16)
    g[c, x, z, ROWS_A:ROWS, :] = fb[...].astype(BF16)
    pl.semaphore_wait(barrier, len(peers))

    for d in range(1, NZ):
        send(g.at[c, x, z], g.at[c, x, z], ("gz", d), at(z_=zs[d]))
    for d in range(1, NY):
        send(columns(ys[d]), pr.at[y], ("p1", d), at(y_=ys[d]))
    for d in range(1, NZ):
        arrived(g.at[c, x, from_z[d]], ("gz", d))
    for d in range(1, NX):
        send(g.at[c, x], g.at[c, x], ("gx", d), at(x_=xs[d]))
    send(g.at[c, x], g.at[c, x], ("gc", 0), sibling)

    def spread(core, xx):
        stg8[...] = g[core, xx].astype(F32)
        for j in range(ROWS):
            w[core * 4 + xx, :, j * LANES : (j + 1) * LANES] = stg8[:, j, :]

    spread(c, x)

    load_own.wait()
    for d in range(1, NY):
        arrived(pr.at[from_y[d]], ("p1", d))
    for yy in range(NY):
        pf[4 * yy : 4 * yy + 4, :] = pr[yy].astype(F32)
    q[y, zh, x, c] = pf[...].astype(BF16)
    send(q.at[y, zh, x, c], q.at[y, zh, x, c], ("p2", 0), at(z_=step(z, 4, NZ)))

    for d in range(1, NX):
        arrived(g.at[c, from_x[d]], ("gx", d))
        send(g.at[c, from_x[d]], g.at[c, from_x[d]], ("gc", d), sibling)
        spread(c, from_x[d])
    arrived(q.at[y, 1 - zh, x, c], ("p2", 0))
    for d in range(1, NX):
        send(q.at[y, :, x, c], q.at[y, :, x, c], ("p3", d), at(x_=xs[d]))
    for d in range(NX):
        arrived(g.at[other, from_x[d]], ("gc", d))
        spread(other, from_x[d])

    load_act.wait()
    load_cot.wait()
    wide = w[...].reshape(RANK, ROWS * LANES).astype(BF16)
    split = ROWS_A * LANES
    low[y, 0:RANK, :] = dot_nt(wide[:, :split], act[...]).astype(BF16)
    low[y, RANK : 2 * RANK, :] = dot_nt(wide[:, split:], cot[...]).astype(BF16)
    for d in range(1, NY):
        send(low.at[y], low.at[y], ("low", d), at(y_=ys[d]))
    for d in range(1, NY):
        arrived(low.at[from_y[d]], ("low", d))
    total = low[0].astype(F32)
    for yy in range(1, NY):
        total = total + low[yy].astype(F32)
    kept = (total * keep_ref[0].astype(F32)).astype(BF16)
    input_kept, grad_kept = kept[0:RANK], kept[RANK : 2 * RANK]

    chunk = 4
    for i in range(ROWS // chunk):
        first = i * chunk
        if first < ROWS_A:
            part = dot_nn(grad_kept, act[:, first * LANES : (first + chunk) * LANES])
        else:
            at_b = first - ROWS_A
            part = dot_nn(input_kept, cot[:, at_b * LANES : (at_b + chunk) * LANES])
        for j in range(chunk):
            stg64[:, first + j, :] = part[:, j * LANES : (j + 1) * LANES]

    order = [1, 2, 3, 0]
    for d in order:
        rows = pl.ds(other * 32 + xs[d] * 8, 8)
        p_send[d] = stg64[rows].astype(BF16)
        send(p_send.at[d], r1.at[d], ("c1", d), sibling)
    for d in range(1, NX):
        arrived(q.at[y, :, from_x[d], c], ("p3", d))
    for d in range(1, NY):
        send(q.at[y, :, :, c], q.at[y, :, :, c], ("p4", d), at(y_=ys[d]))
    send(q.at[y, :, :, c], q.at[y, :, :, c], ("p5", 0), sibling)
    for d in order:
        arrived(r1.at[d], ("c1", d))
        rows = pl.ds(c * 32 + xs[d] * 8, 8)
        pair = stg64[rows] + r1[d].astype(F32)
        if d:
            s2[d] = pair.astype(BF16)
            send(s2.at[d], r2.at[d], ("c2", d), at(x_=xs[d]))
        else:
            t32[...] = pair
    for d in range(1, NX):
        arrived(r2.at[d], ("c2", d))
    column = t32[...]
    for d in range(1, NX):
        column = column + r2[d].astype(F32)
    t32[...] = column
    t16[...] = column.astype(BF16)
    for d in range(1, NZ):
        send(t16.at[zs[d]], r3.at[d], ("c3", d), at(z_=zs[d]))
    for d in range(1, NZ):
        arrived(r3.at[d], ("c3", d))
    grad = t32[z]
    for d in range(1, NZ):
        grad = grad + r3[d].astype(F32)
    grad = grad * (adapter_scale / ROLLOUT_TOKENS)
    grad_out[...] = grad

    new_a, _, _ = adam_update(fa[...], ma[...], va[...], grad[0:ROWS_A])
    ea[x, z] = new_a.astype(BF16)
    for d in range(1, NZ):
        send(ea.at[x, z], ea.at[x, z], ("ez", d), at(z_=zs[d]))
    new_b, _, _ = adam_update(fb[...], mb[...], vb[...], grad[ROWS_A:ROWS])
    blocks = jnp.concatenate(in_wide_blocks(new_b), axis=0).astype(BF16)
    for kk in range(4):
        ebz[z, kk] = blocks[8 * kk : 8 * kk + 8]
    for d in range(1, NZ):
        send(ebz.at[z], ebz.at[z], ("bz", d), at(z_=zs[d]))
    for d in range(1, NZ):
        arrived(ea.at[x, from_z[d]], ("ez", d))
    for d in range(1, NX):
        send(ea.at[x], ea.at[x], ("ex", d), at(x_=xs[d]))
    for d in range(1, NZ):
        arrived(ebz.at[from_z[d]], ("bz", d))

    def two_blocks(xx):
        return ebz.at[:, pl.ds(lax.rem(xx, 2) * 2, 2)]

    for d in range(1, NX):
        send(two_blocks(xs[d]), ebx.at[x], ("bx", d), at(x_=xs[d]))
    ebx[x] = ebz[:, pl.ds(lax.rem(x, 2) * 2, 2)]
    for d in range(1, NX):
        arrived(ea.at[from_x[d]], ("ex", d))
    for xx in range(NX):
        stga[xx * NZ : (xx + 1) * NZ] = ea[xx].astype(F32)
    for j in range(ROWS_A):
        ha[y, c, :, j * LANES : (j + 1) * LANES] = stga[:, j, :].astype(BF16)
    for d in range(1, NY):
        send(ha.at[y, c], ha.at[y, c], ("ey", d), at(y_=ys[d]))
    send(ha.at[y, c], ha.at[y, c], ("ec", 0), sibling)

    for d in range(1, NY):
        arrived(q.at[from_y[d], :, :, c], ("p4", d))
        send(q.at[from_y[d], :, :, c], q.at[from_y[d], :, :, c], ("p5", d), sibling)

    for d in range(1, NX):
        arrived(ebx.at[from_x[d]], ("bx", d))
    send(ebx.at[:, :, other], ebd, ("bc", 0), sibling)
    for xx in range(NX):
        stgb[c, xx * NZ : (xx + 1) * NZ] = ebx[xx, :, c].astype(F32)
    arrived(ebd, ("bc", 0))
    for xx in range(NX):
        stgb[other, xx * NZ : (xx + 1) * NZ] = ebd[xx].astype(F32)
    for yy in range(NY):
        for cc in range(NC):
            for half in range(2):
                bs[yy, cc, :, half * LANES : (half + 1) * LANES] = stgb[
                    cc, :, 2 * yy + half, :
                ].astype(BF16)
    holder = zh * 2 + lax.div(x, 2)
    for d in range(1, NY):
        key = ("by", d)
        one = copy(bs.at[ys[d]], bb, key, at(y_=ys[d]))

        @pl.when(y == holder)
        def _():
            one.start()

    @pl.when(y == holder)
    def _():
        bb[...] = bs[y]

    for d in range(1, NY):
        arrived(ha.at[from_y[d], c], ("ey", d))
        send(ha.at[from_y[d], c], ha.at[from_y[d], c], ("ec", d), sibling)

    for d in range(1, NY):

        @pl.when(from_y[d] == holder)
        def _():
            arrived(bb, ("by", d))

    for d in range(NY):
        arrived(ha.at[from_y[d], other], ("ec", d))
    for d in range(NY):
        arrived(q.at[from_y[d], :, :, other], ("p5", d))
    for one in sent:
        one.wait_send()

    for d in range(1, NY):
        one = copy(bs.at[ys[d]], bb, ("by", d), at(y_=ys[d]))

        @pl.when(y == holder)
        def _():
            one.wait_send()


SEMAPHORES = 96


def exchange(act, cot, keep, fa, ma, va, fb, mb, vb, prompts):
    any_spec = pl.BlockSpec(memory_space=pl.ANY)
    vmem = pl.BlockSpec(memory_space=pltpu.VMEM)
    smem = pl.BlockSpec(memory_space=pltpu.SMEM)
    tokens = act.shape[0]
    return pl.pallas_call(
        exchange_kernel,
        out_shape=(
            jax.ShapeDtypeStruct((ROWS, LANES), F32),
            jax.ShapeDtypeStruct((NY, NC, 32, 2048), BF16),
            jax.ShapeDtypeStruct((NC, 32, WIDE), BF16),
            jax.ShapeDtypeStruct((NY, 2, NX, NC, 16, 2048), BF16),
        ),
        in_specs=[any_spec, any_spec, smem] + [vmem] * 6 + [any_spec],
        out_specs=(vmem, vmem, vmem, vmem),
        scratch_shapes=[
            pltpu.VMEM(act.shape, BF16),
            pltpu.VMEM(cot.shape, BF16),
            pltpu.VMEM((NC, NX, NZ, ROWS, LANES), BF16),
            pltpu.VMEM((NZ, ROWS, LANES), F32),
            pltpu.VMEM((NC * NX, NZ, ROWS * LANES), F32),
            pltpu.VMEM((NY, 2 * RANK, tokens), BF16),
            pltpu.VMEM((RANK, ROWS, LANES), F32),
            pltpu.VMEM((NX, NZ, ROWS, LANES), BF16),
            pltpu.VMEM((NX, NZ, ROWS, LANES), BF16),
            pltpu.VMEM((NX, NZ, ROWS, LANES), BF16),
            pltpu.VMEM((NX, NZ, ROWS, LANES), BF16),
            pltpu.VMEM((NZ, ROWS, LANES), F32),
            pltpu.VMEM((NZ, ROWS, LANES), BF16),
            pltpu.VMEM((NZ, ROWS, LANES), BF16),
            pltpu.VMEM((NX, NZ, ROWS_A, LANES), BF16),
            pltpu.VMEM((NX * NZ, ROWS_A, LANES), F32),
            pltpu.VMEM((NZ, 4, 8, LANES), BF16),
            pltpu.VMEM((NX, NZ, 2, 8, LANES), BF16),
            pltpu.VMEM((NX, NZ, 8, LANES), BF16),
            pltpu.VMEM((NC, NX * NZ, 8, LANES), F32),
            pltpu.VMEM((NY, NC, 32, WIDE), BF16),
            pltpu.VMEM((NY, 4, 2048), BF16),
            pltpu.VMEM((16, 2048), F32),
            pltpu.SemaphoreType.DMA((3,)),
            pltpu.SemaphoreType.DMA((SEMAPHORES,)),
            pltpu.SemaphoreType.DMA((SEMAPHORES,)),
        ],
        compiler_params=pltpu.CompilerParams(
            collective_id=0, has_side_effects=True, vmem_limit_bytes=32 * 1024 * 1024
        ),
        name="exchange",
    )(act, cot, keep, fa, ma, va, fb, mb, vb, prompts)


def merge_kernel(
    base, ha, bb, q, grad, fa, ma, va, fb, mb, vb, ua, ub, na, nb, sa, sb, merged, proj, bt, acc
):
    i = pl.program_id(0)

    @pl.when(i == 0)
    def _():
        bt[...] = bb[...].reshape(RANK, WIDE).astype(F32).T.astype(BF16)
        ua[...], na[...], sa[...] = adam_update(fa[...], ma[...], va[...], grad[0:ROWS_A])
        ub[...], nb[...], sb[...] = adam_update(fb[...], mb[...], vb[...], grad[ROWS_A:ROWS])

    delta = dot_nn(bt[0:BLOCK, :], ha[0].reshape(RANK, 2048))
    rows = (base[...].astype(F32) + adapter_scale * delta).astype(BF16)
    merged[...] = rows
    part = dot_nt(rows, q[0].reshape(256, 2048))

    @pl.when(i == 0)
    def _():
        acc[...] = part

    @pl.when(i > 0)
    def _():
        acc[...] += part

    @pl.when(i == NY - 1)
    def _():
        proj[...] = acc[...].astype(BF16)


def merge(base, ha, bb, q, grad, fa, ma, va, fb, mb, vb):
    whole = pl.BlockSpec(memory_space=pltpu.VMEM)
    sds = jax.ShapeDtypeStruct

    def fixed(shape):
        return pl.BlockSpec(shape, lambda i: (0,) * len(shape))

    a_shape, b_shape = (ROWS_A, LANES), (ROWS_B, LANES)
    return pl.pallas_call(
        merge_kernel,
        grid=(NY,),
        out_shape=(
            sds(a_shape, F32),
            sds(b_shape, F32),
            sds(a_shape, F32),
            sds(b_shape, F32),
            sds(a_shape, F32),
            sds(b_shape, F32),
            sds(base.shape, BF16),
            sds((BLOCK, 256), BF16),
        ),
        in_specs=[
            pl.BlockSpec((BLOCK, 2048), lambda i: (0, i)),
            pl.BlockSpec((1, NC, 32, 2048), lambda i: (i, 0, 0, 0)),
            fixed((NC, 32, WIDE)),
            pl.BlockSpec((1, 2, NX, NC, 16, 2048), lambda i: (i, 0, 0, 0, 0, 0)),
            fixed((ROWS, LANES)),
        ]
        + [fixed(a_shape)] * 3
        + [fixed(b_shape)] * 3,
        out_specs=[
            fixed(a_shape),
            fixed(b_shape),
            fixed(a_shape),
            fixed(b_shape),
            fixed(a_shape),
            fixed(b_shape),
            pl.BlockSpec((BLOCK, 2048), lambda i: (0, i)),
            fixed((BLOCK, 256)),
        ],
        scratch_shapes=[pltpu.VMEM((WIDE, RANK), BF16), pltpu.VMEM((BLOCK, 256), F32)],
        compiler_params=pltpu.CompilerParams(
            dimension_semantics=("arbitrary",), vmem_limit_bytes=32 * 1024 * 1024
        ),
        name="merge",
    )(base, ha, bb, q, grad, fa, ma, va, fb, mb, vb)


def body(
    activations,
    cotangent,
    block_keep,
    input_factor,
    input_mean,
    input_square,
    output_factor,
    output_mean,
    output_square,
    frozen_base_rows,
    prompts,
):
    fa, ma, va = (v.reshape(ROWS_A, LANES) for v in (input_factor, input_mean, input_square))
    fb, mb, vb = (v.reshape(ROWS_B, LANES) for v in (output_factor, output_mean, output_square))
    grad, ha, bb, q = exchange(
        activations, cotangent, block_keep, fa, ma, va, fb, mb, vb, prompts
    )
    ua, ub, na, nb, sa, sb, merged, projected = merge(
        frozen_base_rows, ha, bb, q, grad, fa, ma, va, fb, mb, vb
    )
    return (
        ua.reshape(1, -1),
        ub.reshape(1, -1),
        na.reshape(1, -1),
        nb.reshape(1, -1),
        sa.reshape(1, -1),
        sb.reshape(1, -1),
        merged,
        projected,
    )


def solution(mesh):
    row = P(("role", "dp"), "tp")
    placed = (
        row,
        row,
        P(("role", "dp")),
        row,
        row,
        row,
        row,
        row,
        row,
        P(("dp", "tp"), None),
        P(("role", "dp", "tp"), None),
    )
    return jax.shard_map(
        body,
        mesh=mesh,
        in_specs=placed,
        out_specs=(
            row,
            row,
            row,
            row,
            row,
            row,
            P(("dp", "tp"), None),
            P(("dp", "tp"), "role"),
        ),
        check_vma=False,
    )
```

```python
import jax
import jax.numpy as jnp
from jax import lax
from jax.experimental import pallas as pl
from jax.experimental.pallas import tpu as pltpu
from jax.sharding import PartitionSpec as P

ROLLOUT_TOKENS = 256
RANK = 64
LANES = 128
ROWS_A, ROWS_B = 16, 28
ROWS = ROWS_A + ROWS_B
NX, NY, NZ, NC = 4, 4, 8, 2
BLOCK = 224
WIDE = 256

adapter_scale = 2.0
learn_rate = 0.004
beta_one = 0.9
beta_two = 0.95
epsilon = 1e-08
first_fix = 1.0 - 0.9**20
second_fix = 1.0 - 0.95**20

F32, BF16 = jnp.float32, jnp.bfloat16
MESH = pl.DeviceIdType.MESH


def adam_update(factor, moment, square, gradient):
    moment_new = beta_one * moment + (1.0 - beta_one) * gradient
    square_new = beta_two * square + (1.0 - beta_two) * gradient * gradient
    factor_new = factor - learn_rate * (moment_new / first_fix) / (
        jnp.sqrt(square_new / second_fix) + epsilon
    )
    return (factor_new, moment_new, square_new)


def dot_nn(a, b):
    return lax.dot_general(a, b, (((1,), (0,)), ((), ())), preferred_element_type=F32)


def dot_nt(a, b):
    return lax.dot_general(a, b, (((1,), (1,)), ((), ())), preferred_element_type=F32)


def in_wide_blocks(rows):
    lane = lax.broadcasted_iota(jnp.int32, (1, LANES), 1)
    rolled = {0: rows}
    for off in (32, 64, 96):
        rolled[off] = pltpu.roll(rows, LANES - off, 1)
    out = []
    for k in range(16):
        row, off = divmod(BLOCK * k, LANES)
        turned = rolled[off]
        for half in range(2):
            first = turned[row + half : row + half + 1]
            if off == 0:
                out.append(first)
                continue
            last = min(row + half + 1, ROWS_B - 1)
            second = turned[last : last + 1]
            out.append(jnp.where(lane < LANES - off, first, second))
    return out


def exchange_kernel(
    act_hbm,
    cot_hbm,
    keep_ref,
    fa_hbm,
    ma_hbm,
    va_hbm,
    fb_hbm,
    mb_hbm,
    vb_hbm,
    prompts_hbm,
    grad_out,
    ha,
    bb,
    q,
    act,
    cot,
    fa,
    ma,
    va,
    fb,
    mb,
    vb,
    g,
    stg8,
    w,
    low,
    stg64,
    p_send,
    r1,
    s2,
    r2,
    t32,
    t16,
    r3,
    ea,
    stga,
    ebz,
    ebx,
    ebd,
    stgb,
    bs,
    pr,
    pf,
    loc,
    ssem,
    rsem,
):
    z_lo = lax.axis_index("role")
    dp = lax.axis_index("dp")
    y = lax.axis_index("tp")
    c = lax.rem(dp, 2)
    x = lax.rem(lax.div(dp, 2), 4)
    zh = lax.div(dp, 8)
    z = zh * 4 + z_lo

    def at(x_=x, y_=y, z_=z, c_=c):
        return {
            "role": lax.rem(z_, 4),
            "dp": lax.div(z_, 4) * 8 + x_ * 2 + c_,
            "tp": y_,
        }

    def step(v, d, n):
        return lax.rem(v + d, n)

    other = 1 - c
    sibling = at(c_=other)
    xs = [step(x, d, NX) for d in range(NX)]
    ys = [step(y, d, NY) for d in range(NY)]
    zs = [step(z, d, NZ) for d in range(NZ)]
    from_x = [step(x, NX - d, NX) for d in range(NX)]
    from_y = [step(y, NY - d, NY) for d in range(NY)]
    from_z = [step(z, NZ - d, NZ) for d in range(NZ)]

    names = {}

    def copy(src, dst, key, device):
        i = names.setdefault(key, len(names))
        return pltpu.make_async_remote_copy(
            src_ref=src,
            dst_ref=dst,
            send_sem=ssem.at[i],
            recv_sem=rsem.at[i],
            device_id=device,
            device_id_type=MESH,
        )

    sent = []

    def send(src, dst, key, device):
        one = copy(src, dst, key, device)
        one.start()
        sent.append(one)

    def arrived(dst, key):
        copy(dst, dst, key, sibling).wait_recv()

    load_act = pltpu.make_async_copy(act_hbm, act, loc.at[0])
    load_cot = pltpu.make_async_copy(cot_hbm, cot, loc.at[1])
    loads = [
        pltpu.make_async_copy(src, dst, loc.at[3 + i])
        for i, (src, dst) in enumerate(
            ((fa_hbm, fa), (fb_hbm, fb), (ma_hbm, ma), (va_hbm, va), (mb_hbm, mb), (vb_hbm, vb))
        )
    ]
    for one in loads[:2]:
        one.start()
    quarter = 2048

    def columns(yy):
        return prompts_hbm.at[:, pl.ds(pl.multiple_of(yy * quarter, quarter), quarter)]

    load_own = pltpu.make_async_copy(columns(y), pr.at[y], loc.at[2])
    load_own.start()
    load_act.start()
    load_cot.start()
    for one in loads[2:]:
        one.start()

    barrier = pltpu.get_barrier_semaphore()
    peers = (
        [sibling]
        + [at(x_=v) for v in xs[1:]]
        + [at(y_=v) for v in ys[1:]]
        + [at(z_=v) for v in zs[1:]]
    )
    for peer in peers:
        pl.semaphore_signal(barrier, inc=1, device_id=peer, device_id_type=MESH)

    for one in loads[:2]:
        one.wait()
    g[c, x, z, 0:ROWS_A, :] = fa[:, 0, :].astype(BF16)
    g[c, x, z, ROWS_A:ROWS, :] = fb[:, 0, :].astype(BF16)
    pl.semaphore_wait(barrier, len(peers))

    for d in range(1, NZ):
        send(g.at[c, x, z], g.at[c, x, z], ("gz", d), at(z_=zs[d]))
    for d in range(1, NY):
        send(columns(ys[d]), pr.at[y], ("p1", d), at(y_=ys[d]))
    for d in range(1, NZ):
        arrived(g.at[c, x, from_z[d]], ("gz", d))
    for d in range(1, NX):
        send(g.at[c, x], g.at[c, x], ("gx", d), at(x_=xs[d]))
    send(g.at[c, x], g.at[c, x], ("gc", 0), sibling)

    def spread(core, xx):
        stg8[...] = g[core, xx].astype(F32)
        for j in range(ROWS):
            w[core * 4 + xx, :, j * LANES : (j + 1) * LANES] = stg8[:, j, :]

    spread(c, x)

    load_own.wait()
    for d in range(1, NY):
        arrived(pr.at[from_y[d]], ("p1", d))
    for yy in range(NY):
        pf[4 * yy : 4 * yy + 4, :] = pr[yy].astype(F32)
    q[y, zh, x, c] = pf[...].astype(BF16)
    send(q.at[y, zh, x, c], q.at[y, zh, x, c], ("p2", 0), at(z_=step(z, 4, NZ)))

    for d in range(1, NX):
        arrived(g.at[c, from_x[d]], ("gx", d))
        send(g.at[c, from_x[d]], g.at[c, from_x[d]], ("gc", d), sibling)
        spread(c, from_x[d])
    arrived(q.at[y, 1 - zh, x, c], ("p2", 0))
    for d in range(1, NX):
        send(q.at[y, :, x, c], q.at[y, :, x, c], ("p3", d), at(x_=xs[d]))
    for d in range(NX):
        arrived(g.at[other, from_x[d]], ("gc", d))
        spread(other, from_x[d])

    load_act.wait()
    load_cot.wait()
    for one in loads[2:]:
        one.wait()
    wide = w[...].reshape(RANK, ROWS * LANES).astype(BF16)
    split = ROWS_A * LANES
    low[y, 0:RANK, :] = dot_nt(wide[:, :split], act[...]).astype(BF16)
    low[y, RANK : 2 * RANK, :] = dot_nt(wide[:, split:], cot[...]).astype(BF16)
    for d in range(1, NY):
        send(low.at[y], low.at[y], ("low", d), at(y_=ys[d]))
    for d in range(1, NY):
        arrived(low.at[from_y[d]], ("low", d))
    total = low[0].astype(F32)
    for yy in range(1, NY):
        total = total + low[yy].astype(F32)
    kept = (total * keep_ref[0].astype(F32)).astype(BF16)
    input_kept, grad_kept = kept[0:RANK], kept[RANK : 2 * RANK]

    chunk = 4
    for i in range(ROWS // chunk):
        first = i * chunk
        if first < ROWS_A:
            part = dot_nn(grad_kept, act[:, first * LANES : (first + chunk) * LANES])
        else:
            at_b = first - ROWS_A
            part = dot_nn(input_kept, cot[:, at_b * LANES : (at_b + chunk) * LANES])
        for j in range(chunk):
            stg64[:, first + j, :] = part[:, j * LANES : (j + 1) * LANES]

    order = [1, 2, 3, 0]
    for d in order:
        rows = pl.ds(other * 32 + xs[d] * 8, 8)
        p_send[d] = stg64[rows].astype(BF16)
        send(p_send.at[d], r1.at[d], ("c1", d), sibling)
    for d in range(1, NX):
        arrived(q.at[y, :, from_x[d], c], ("p3", d))
    for d in range(1, NY):
        send(q.at[y, :, :, c], q.at[y, :, :, c], ("p4", d), at(y_=ys[d]))
    send(q.at[y, :, :, c], q.at[y, :, :, c], ("p5", 0), sibling)
    for d in order:
        arrived(r1.at[d], ("c1", d))
        rows = pl.ds(c * 32 + xs[d] * 8, 8)
        pair = stg64[rows] + r1[d].astype(F32)
        if d:
            s2[d] = pair.astype(BF16)
            send(s2.at[d], r2.at[d], ("c2", d), at(x_=xs[d]))
        else:
            t32[...] = pair
    for d in range(1, NX):
        arrived(r2.at[d], ("c2", d))
    column = t32[...]
    for d in range(1, NX):
        column = column + r2[d].astype(F32)
    t32[...] = column
    t16[...] = column.astype(BF16)
    for d in range(1, NZ):
        send(t16.at[zs[d]], r3.at[d], ("c3", d), at(z_=zs[d]))
    for d in range(1, NZ):
        arrived(r3.at[d], ("c3", d))
    grad = t32[z]
    for d in range(1, NZ):
        grad = grad + r3[d].astype(F32)
    grad = grad * (adapter_scale / ROLLOUT_TOKENS)
    grad_out[...] = grad

    new_a, _, _ = adam_update(fa[:, 0, :], ma[:, 0, :], va[:, 0, :], grad[0:ROWS_A])
    ea[x, z] = new_a.astype(BF16)
    for d in range(1, NZ):
        send(ea.at[x, z], ea.at[x, z], ("ez", d), at(z_=zs[d]))
    new_b, _, _ = adam_update(fb[:, 0, :], mb[:, 0, :], vb[:, 0, :], grad[ROWS_A:ROWS])
    blocks = jnp.concatenate(in_wide_blocks(new_b), axis=0).astype(BF16)
    for kk in range(4):
        ebz[z, kk] = blocks[8 * kk : 8 * kk + 8]
    for d in range(1, NZ):
        send(ebz.at[z], ebz.at[z], ("bz", d), at(z_=zs[d]))
    for d in range(1, NZ):
        arrived(ea.at[x, from_z[d]], ("ez", d))
    for d in range(1, NX):
        send(ea.at[x], ea.at[x], ("ex", d), at(x_=xs[d]))
    for d in range(1, NZ):
        arrived(ebz.at[from_z[d]], ("bz", d))

    def two_blocks(xx):
        return ebz.at[:, pl.ds(lax.rem(xx, 2) * 2, 2)]

    for d in range(1, NX):
        send(two_blocks(xs[d]), ebx.at[x], ("bx", d), at(x_=xs[d]))
    ebx[x] = ebz[:, pl.ds(lax.rem(x, 2) * 2, 2)]
    for d in range(1, NX):
        arrived(ea.at[from_x[d]], ("ex", d))
    for xx in range(NX):
        stga[xx * NZ : (xx + 1) * NZ] = ea[xx].astype(F32)
    for j in range(ROWS_A):
        ha[y, c, :, j * LANES : (j + 1) * LANES] = stga[:, j, :].astype(BF16)
    for d in range(1, NY):
        send(ha.at[y, c], ha.at[y, c], ("ey", d), at(y_=ys[d]))
    send(ha.at[y, c], ha.at[y, c], ("ec", 0), sibling)

    for d in range(1, NY):
        arrived(q.at[from_y[d], :, :, c], ("p4", d))
        send(q.at[from_y[d], :, :, c], q.at[from_y[d], :, :, c], ("p5", d), sibling)

    for d in range(1, NX):
        arrived(ebx.at[from_x[d]], ("bx", d))
    send(ebx.at[:, :, other], ebd, ("bc", 0), sibling)
    for xx in range(NX):
        stgb[c, xx * NZ : (xx + 1) * NZ] = ebx[xx, :, c].astype(F32)
    arrived(ebd, ("bc", 0))
    for xx in range(NX):
        stgb[other, xx * NZ : (xx + 1) * NZ] = ebd[xx].astype(F32)
    for yy in range(NY):
        for cc in range(NC):
            for half in range(2):
                bs[yy, cc, :, half * LANES : (half + 1) * LANES] = stgb[
                    cc, :, 2 * yy + half, :
                ].astype(BF16)
    holder = zh * 2 + lax.div(x, 2)
    for d in range(1, NY):
        key = ("by", d)
        one = copy(bs.at[ys[d]], bb, key, at(y_=ys[d]))

        @pl.when(y == holder)
        def _():
            one.start()

    @pl.when(y == holder)
    def _():
        bb[...] = bs[y]

    for d in range(1, NY):
        arrived(ha.at[from_y[d], c], ("ey", d))
        send(ha.at[from_y[d], c], ha.at[from_y[d], c], ("ec", d), sibling)

    for d in range(1, NY):

        @pl.when(from_y[d] == holder)
        def _():
            arrived(bb, ("by", d))

    for d in range(NY):
        arrived(ha.at[from_y[d], other], ("ec", d))
    for d in range(NY):
        arrived(q.at[from_y[d], :, :, other], ("p5", d))
    for one in sent:
        one.wait_send()

    for d in range(1, NY):
        one = copy(bs.at[ys[d]], bb, ("by", d), at(y_=ys[d]))

        @pl.when(y == holder)
        def _():
            one.wait_send()


SEMAPHORES = 96


def in_hbm(array):
    return pltpu.with_memory_space_constraint(array, pltpu.HBM)


def exchange(act, cot, keep, fa, ma, va, fb, mb, vb, prompts):
    hbm = pl.BlockSpec(memory_space=pltpu.HBM)
    vmem = pl.BlockSpec(memory_space=pltpu.VMEM)
    smem = pl.BlockSpec(memory_space=pltpu.SMEM)
    tokens = act.shape[0]
    return pl.pallas_call(
        exchange_kernel,
        out_shape=(
            jax.ShapeDtypeStruct((ROWS, LANES), F32),
            jax.ShapeDtypeStruct((NY, NC, 32, 2048), BF16),
            jax.ShapeDtypeStruct((NC, 32, WIDE), BF16),
            jax.ShapeDtypeStruct((NY, 2, NX, NC, 16, 2048), BF16),
        ),
        in_specs=[hbm, hbm, smem] + [hbm] * 7,
        out_specs=(vmem, vmem, vmem, vmem),
        scratch_shapes=[
            pltpu.VMEM(act.shape, BF16),
            pltpu.VMEM(cot.shape, BF16),
            pltpu.VMEM(fa.shape, F32),
            pltpu.VMEM(fa.shape, F32),
            pltpu.VMEM(fa.shape, F32),
            pltpu.VMEM(fb.shape, F32),
            pltpu.VMEM(fb.shape, F32),
            pltpu.VMEM(fb.shape, F32),
            pltpu.VMEM((NC, NX, NZ, ROWS, LANES), BF16),
            pltpu.VMEM((NZ, ROWS, LANES), F32),
            pltpu.VMEM((NC * NX, NZ, ROWS * LANES), F32),
            pltpu.VMEM((NY, 2 * RANK, tokens), BF16),
            pltpu.VMEM((RANK, ROWS, LANES), F32),
            pltpu.VMEM((NX, NZ, ROWS, LANES), BF16),
            pltpu.VMEM((NX, NZ, ROWS, LANES), BF16),
            pltpu.VMEM((NX, NZ, ROWS, LANES), BF16),
            pltpu.VMEM((NX, NZ, ROWS, LANES), BF16),
            pltpu.VMEM((NZ, ROWS, LANES), F32),
            pltpu.VMEM((NZ, ROWS, LANES), BF16),
            pltpu.VMEM((NZ, ROWS, LANES), BF16),
            pltpu.VMEM((NX, NZ, ROWS_A, LANES), BF16),
            pltpu.VMEM((NX * NZ, ROWS_A, LANES), F32),
            pltpu.VMEM((NZ, 4, 8, LANES), BF16),
            pltpu.VMEM((NX, NZ, 2, 8, LANES), BF16),
            pltpu.VMEM((NX, NZ, 8, LANES), BF16),
            pltpu.VMEM((NC, NX * NZ, 8, LANES), F32),
            pltpu.VMEM((NY, NC, 32, WIDE), BF16),
            pltpu.VMEM((NY, 4, 2048), BF16),
            pltpu.VMEM((16, 2048), F32),
            pltpu.SemaphoreType.DMA((9,)),
            pltpu.SemaphoreType.DMA((SEMAPHORES,)),
            pltpu.SemaphoreType.DMA((SEMAPHORES,)),
        ],
        compiler_params=pltpu.CompilerParams(
            collective_id=0, has_side_effects=True, vmem_limit_bytes=32 * 1024 * 1024
        ),
        cost_estimate=pl.CostEstimate(
            flops=200_000_000_000, bytes_accessed=8_000_000, transcendentals=0
        ),
        name="exchange",
    )(in_hbm(act), in_hbm(cot), keep, *map(in_hbm, (fa, ma, va, fb, mb, vb)), in_hbm(prompts))


def merge_kernel(
    base, ha, bb, q, grad, fa, ma, va, fb, mb, vb, ua, ub, na, nb, sa, sb, merged, proj, bt, acc
):
    i = pl.program_id(0)

    @pl.when(i == 0)
    def _():
        bt[...] = bb[...].reshape(RANK, WIDE).astype(F32).T.astype(BF16)
        ua[:, 0, :], na[:, 0, :], sa[:, 0, :] = adam_update(
            fa[:, 0, :], ma[:, 0, :], va[:, 0, :], grad[0:ROWS_A]
        )
        ub[:, 0, :], nb[:, 0, :], sb[:, 0, :] = adam_update(
            fb[:, 0, :], mb[:, 0, :], vb[:, 0, :], grad[ROWS_A:ROWS]
        )

    delta = dot_nn(bt[0:BLOCK, :], ha[0].reshape(RANK, 2048))
    rows = (base[...].astype(F32) + adapter_scale * delta).astype(BF16)
    merged[...] = rows
    part = dot_nt(rows, q[0].reshape(256, 2048))

    @pl.when(i == 0)
    def _():
        acc[...] = part

    @pl.when(i > 0)
    def _():
        acc[...] += part

    @pl.when(i == NY - 1)
    def _():
        proj[...] = acc[...].astype(BF16)


def merge(base, ha, bb, q, grad, fa, ma, va, fb, mb, vb):
    whole = pl.BlockSpec(memory_space=pltpu.VMEM)
    sds = jax.ShapeDtypeStruct

    def fixed(shape):
        return pl.BlockSpec(shape, lambda i: (0,) * len(shape))

    a_shape, b_shape = (ROWS_A, 1, LANES), (ROWS_B, 1, LANES)
    return pl.pallas_call(
        merge_kernel,
        grid=(NY,),
        out_shape=(
            sds(a_shape, F32),
            sds(b_shape, F32),
            sds(a_shape, F32),
            sds(b_shape, F32),
            sds(a_shape, F32),
            sds(b_shape, F32),
            sds(base.shape, BF16),
            sds((BLOCK, 256), BF16),
        ),
        in_specs=[
            pl.BlockSpec((BLOCK, 2048), lambda i: (0, i)),
            pl.BlockSpec((1, NC, 32, 2048), lambda i: (i, 0, 0, 0)),
            fixed((NC, 32, WIDE)),
            pl.BlockSpec((1, 2, NX, NC, 16, 2048), lambda i: (i, 0, 0, 0, 0, 0)),
            fixed((ROWS, LANES)),
        ]
        + [fixed(a_shape)] * 3
        + [fixed(b_shape)] * 3,
        out_specs=[
            fixed(a_shape),
            fixed(b_shape),
            fixed(a_shape),
            fixed(b_shape),
            fixed(a_shape),
            fixed(b_shape),
            pl.BlockSpec((BLOCK, 2048), lambda i: (0, i)),
            fixed((BLOCK, 256)),
        ],
        scratch_shapes=[pltpu.VMEM((WIDE, RANK), BF16), pltpu.VMEM((BLOCK, 256), F32)],
        compiler_params=pltpu.CompilerParams(
            dimension_semantics=("arbitrary",), vmem_limit_bytes=32 * 1024 * 1024
        ),
        name="merge",
    )(base, ha, bb, q, grad, fa, ma, va, fb, mb, vb)


def body(
    activations,
    cotangent,
    block_keep,
    input_factor,
    input_mean,
    input_square,
    output_factor,
    output_mean,
    output_square,
    frozen_base_rows,
    prompts,
):
    fa, ma, va = (v.reshape(ROWS_A, 1, LANES) for v in (input_factor, input_mean, input_square))
    fb, mb, vb = (v.reshape(ROWS_B, 1, LANES) for v in (output_factor, output_mean, output_square))
    grad, ha, bb, q = exchange(
        activations, cotangent, block_keep, fa, ma, va, fb, mb, vb, prompts
    )
    ua, ub, na, nb, sa, sb, merged, projected = merge(
        frozen_base_rows, ha, bb, q, grad, fa, ma, va, fb, mb, vb
    )
    return (
        ua.reshape(1, -1),
        ub.reshape(1, -1),
        na.reshape(1, -1),
        nb.reshape(1, -1),
        sa.reshape(1, -1),
        sb.reshape(1, -1),
        merged,
        projected,
    )


def solution(mesh):
    row = P(("role", "dp"), "tp")
    placed = (
        row,
        row,
        P(("role", "dp")),
        row,
        row,
        row,
        row,
        row,
        row,
        P(("dp", "tp"), None),
        P(("role", "dp", "tp"), None),
    )
    return jax.shard_map(
        body,
        mesh=mesh,
        in_specs=placed,
        out_specs=(
            row,
            row,
            row,
            row,
            row,
            row,
            P(("dp", "tp"), None),
            P(("dp", "tp"), "role"),
        ),
        check_vma=False,
    )
```

```python
import jax
import jax.numpy as jnp
from jax import lax
from jax.experimental import pallas as pl
from jax.experimental.pallas import tpu as pltpu
from jax.sharding import PartitionSpec as P

ROLLOUT_TOKENS = 256
RANK = 64
LANES = 128
ROWS_A, ROWS_B = 16, 28
ROWS = ROWS_A + ROWS_B
NX, NY, NZ, NC = 4, 4, 8, 2
BLOCK = 224
WIDE = 256
HALF, PART = 4096, 1024

adapter_scale = 2.0
learn_rate = 0.004
beta_one = 0.9
beta_two = 0.95
epsilon = 1e-08
first_fix = 1.0 - 0.9**20
second_fix = 1.0 - 0.95**20

F32, BF16 = jnp.float32, jnp.bfloat16
MESH = pl.DeviceIdType.MESH


def adam_update(factor, moment, square, gradient):
    moment_new = beta_one * moment + (1.0 - beta_one) * gradient
    square_new = beta_two * square + (1.0 - beta_two) * gradient * gradient
    factor_new = factor - learn_rate * (moment_new / first_fix) / (
        jnp.sqrt(square_new / second_fix) + epsilon
    )
    return (factor_new, moment_new, square_new)


def dot_nn(a, b):
    return lax.dot_general(a, b, (((1,), (0,)), ((), ())), preferred_element_type=F32)


def dot_nt(a, b):
    return lax.dot_general(a, b, (((1,), (1,)), ((), ())), preferred_element_type=F32)


def in_wide_blocks(rows):
    lane = lax.broadcasted_iota(jnp.int32, (1, LANES), 1)
    rolled = {0: rows}
    for off in (32, 64, 96):
        rolled[off] = pltpu.roll(rows, LANES - off, 1)
    out = []
    for k in range(16):
        row, off = divmod(BLOCK * k, LANES)
        turned = rolled[off]
        for half in range(2):
            first = turned[row + half : row + half + 1]
            if off == 0:
                out.append(first)
                continue
            last = min(row + half + 1, ROWS_B - 1)
            second = turned[last : last + 1]
            out.append(jnp.where(lane < LANES - off, first, second))
    return out


def exchange_kernel(
    act_hbm,
    cot_hbm,
    keep_ref,
    fa_hbm,
    ma_hbm,
    va_hbm,
    fb_hbm,
    mb_hbm,
    vb_hbm,
    prompts_hbm,
    base_hbm,
    grad_out,
    ha0,
    ha1,
    bb,
    part_out,
    q1,
    q2,
    base,
    act,
    cot,
    fa,
    ma,
    va,
    fb,
    mb,
    vb,
    ga,
    gb,
    stg32,
    stg8,
    wa,
    wb,
    low,
    sa,
    sb,
    pa,
    pb,
    r1a,
    r1b,
    f2a,
    s2a,
    s2b,
    r2a,
    r2b,
    t32a,
    t32b,
    t16a,
    t16b,
    r3a,
    r3b,
    ez,
    ea0,
    ea1,
    stga,
    stgy,
    ebz,
    ebx,
    ebd,
    stgb,
    bs,
    pr1,
    pr2,
    pf1,
    pf2,
    loc,
    ssem,
    rsem,
):
    z_lo = lax.axis_index("role")
    dp = lax.axis_index("dp")
    y = lax.axis_index("tp")
    c = lax.rem(dp, 2)
    x = lax.rem(lax.div(dp, 2), 4)
    zh = lax.div(dp, 8)
    z = zh * 4 + z_lo

    def at(x_=x, y_=y, z_=z, c_=c):
        return {
            "role": lax.rem(z_, 4),
            "dp": lax.div(z_, 4) * 8 + x_ * 2 + c_,
            "tp": y_,
        }

    def step(v, d, n):
        return lax.rem(v + d, n)

    other = 1 - c
    sibling = at(c_=other)
    xs = [step(x, d, NX) for d in range(NX)]
    ys = [step(y, d, NY) for d in range(NY)]
    zs = [step(z, d, NZ) for d in range(NZ)]
    from_x = [step(x, NX - d, NX) for d in range(NX)]
    from_y = [step(y, NY - d, NY) for d in range(NY)]
    from_z = [step(z, NZ - d, NZ) for d in range(NZ)]

    names = {}

    def copy(src, dst, key, device):
        i = names.setdefault(key, len(names))
        return pltpu.make_async_remote_copy(
            src_ref=src,
            dst_ref=dst,
            send_sem=ssem.at[i],
            recv_sem=rsem.at[i],
            device_id=device,
            device_id_type=MESH,
        )

    sent = []

    def send(src, dst, key, device):
        one = copy(src, dst, key, device)
        one.start()
        sent.append((key[0], None, one))

    def drain(*kinds):
        for name, condition, one in [e for e in sent if not kinds or e[0] in kinds]:
            if condition is None:
                one.wait_send()
            else:
                pl.when(condition)(one.wait_send)
        sent[:] = [e for e in sent if kinds and e[0] not in kinds]

    def arrived(dst, key):
        copy(dst, dst, key, sibling).wait_recv()

    load_act = pltpu.make_async_copy(act_hbm, act, loc.at[0])
    load_cot = pltpu.make_async_copy(cot_hbm, cot, loc.at[1])
    loads = [
        pltpu.make_async_copy(src, dst, loc.at[3 + i])
        for i, (src, dst) in enumerate(
            ((fa_hbm, fa), (fb_hbm, fb), (ma_hbm, ma), (va_hbm, va), (mb_hbm, mb), (vb_hbm, vb))
        )
    ]
    for one in loads[:2]:
        one.start()

    def late(yy):
        return prompts_hbm.at[:, pl.ds(pl.multiple_of(HALF + yy * PART, PART), PART)]

    early = prompts_hbm.at[:, 0:HALF]
    load_early = pltpu.make_async_copy(early, pr1.at[y], loc.at[2])
    load_late = pltpu.make_async_copy(late(y), pr2.at[y], loc.at[9])
    load_base = pltpu.make_async_copy(base_hbm, base, loc.at[10])
    load_early.start()
    load_late.start()
    load_act.start()
    load_cot.start()
    for one in loads[2:]:
        one.start()
    load_base.start()

    barrier = pltpu.get_barrier_semaphore()
    peers = (
        [sibling]
        + [at(x_=v) for v in xs[1:]]
        + [at(y_=v) for v in ys[1:]]
        + [at(z_=v) for v in zs[1:]]
    )
    for peer in peers:
        pl.semaphore_signal(barrier, inc=1, device_id=peer, device_id_type=MESH)

    for one in loads[:2]:
        one.wait()
    ga[c, x, z] = fa[:, 0, :].astype(BF16)
    gb[c, x, z] = fb[:, 0, :].astype(BF16)
    pl.semaphore_wait(barrier, len(peers))

    for d in range(1, NX):
        send(ga.at[c, x, z], ga.at[c, x, z], ("gax", d), at(x_=xs[d]))
    for d in range(1, NZ):
        send(gb.at[c, x, z], gb.at[c, x, z], ("gbz", d), at(z_=zs[d]))
    for d in range(1, NY):
        send(late(ys[d]), pr2.at[y], ("p1b", d), at(y_=ys[d]))
    for d in range(1, NY):
        send(early, pr1.at[y], ("p1a", d), at(y_=ys[d]))
    for d in range(1, NX):
        arrived(ga.at[c, from_x[d], z], ("gax", d))
    for d in range(1, NZ):
        send(ga.at[c, :, z], ga.at[c, :, z], ("gaz", d), at(z_=zs[d]))
    for d in range(1, NZ):
        arrived(gb.at[c, x, from_z[d]], ("gbz", d))
    for d in range(1, NX):
        send(gb.at[c, x], gb.at[c, x], ("gbx", d), at(x_=xs[d]))
    send(gb.at[c, x], gb.at[c, x], ("gbc", 0), sibling)

    def spread_a(core):
        stg32[...] = ga[core].reshape(32, ROWS_A, LANES).astype(F32)
        for j in range(ROWS_A):
            wa[core, :, j * LANES : (j + 1) * LANES] = stg32[:, j, :]

    def spread_b(core, xx):
        stg8[...] = gb[core, xx].astype(F32)
        for j in range(ROWS_B):
            wb[core * 4 + xx, :, j * LANES : (j + 1) * LANES] = stg8[:, j, :]

    spread_b(c, x)

    z_pair = at(z_=step(z, 4, NZ))
    load_late.wait()
    for d in range(1, NY):
        arrived(pr2.at[from_y[d]], ("p1b", d))
    for yy in range(NY):
        pf2[4 * yy : 4 * yy + 4, :] = pr2[yy].astype(F32)
    q2[y, zh, x, c] = pf2[...].astype(BF16)
    load_early.wait()
    for d in range(1, NY):
        arrived(pr1.at[from_y[d]], ("p1a", d))
    for yy in range(NY):
        pf1[4 * yy : 4 * yy + 4, :] = pr1[yy].astype(F32)
    q1[zh, x, c] = pf1[...].astype(BF16)

    for d in range(1, NZ):
        arrived(ga.at[c, :, from_z[d]], ("gaz", d))
    send(ga.at[c], ga.at[c], ("gac", 0), sibling)
    send(q2.at[y, zh, x, c], q2.at[y, zh, x, c], ("p2b", 0), z_pair)
    spread_a(c)
    for d in range(1, NX):
        arrived(gb.at[c, from_x[d]], ("gbx", d))
        send(gb.at[c, from_x[d]], gb.at[c, from_x[d]], ("gbc", d), sibling)
        spread_b(c, from_x[d])
    arrived(ga.at[other], ("gac", 0))
    send(q1.at[zh, x, c], q1.at[zh, x, c], ("p2a", 0), z_pair)
    spread_a(other)
    for d in range(NX):
        arrived(gb.at[other, from_x[d]], ("gbc", d))
        spread_b(other, from_x[d])

    load_act.wait()
    load_cot.wait()
    for one in loads[2:]:
        one.wait()
    wide_a = wa[...].reshape(RANK, ROWS_A * LANES).astype(BF16)
    wide_b = wb[...].reshape(RANK, ROWS_B * LANES).astype(BF16)
    low[y, 0:RANK, :] = dot_nt(wide_a, act[...]).astype(BF16)
    low[y, RANK : 2 * RANK, :] = dot_nt(wide_b, cot[...]).astype(BF16)
    for d in range(1, NY):
        send(low.at[y], low.at[y], ("low", d), at(y_=ys[d]))
    arrived(q2.at[y, 1 - zh, x, c], ("p2b", 0))
    for d in range(1, NX):
        send(q2.at[y, :, x, c], q2.at[y, :, x, c], ("p3b", d), at(x_=xs[d]))
    for d in range(1, NX):
        send(q1.at[zh, x, c], q1.at[zh, x, c], ("p3a", d), at(x_=xs[d]))
    drain("gax", "gaz", "gac", "gbz", "gbx", "gbc", "p1a", "p1b")
    for d in range(1, NY):
        arrived(low.at[from_y[d]], ("low", d))
    total = low[0].astype(F32)
    for yy in range(1, NY):
        total = total + low[yy].astype(F32)
    kept = (total * keep_ref[0].astype(F32)).astype(BF16)
    input_kept, grad_kept = kept[0:RANK], kept[RANK : 2 * RANK]

    chunk = 4
    for first in range(0, ROWS_A, chunk):
        part = dot_nn(grad_kept, act[:, first * LANES : (first + chunk) * LANES])
        for j in range(chunk):
            sa[:, first + j, :] = part[:, j * LANES : (j + 1) * LANES]
    mine, theirs = pl.ds(c * 32, 32), pl.ds(other * 32, 32)
    pa[...] = sa[theirs].reshape(NX, NZ, ROWS_A, LANES).astype(BF16)
    send(pa, r1a, ("c1a", 0), sibling)
    for first in range(0, ROWS_B, chunk):
        part = dot_nn(input_kept, cot[:, first * LANES : (first + chunk) * LANES])
        for j in range(chunk):
            sb[:, first + j, :] = part[:, j * LANES : (j + 1) * LANES]

    order = [1, 2, 3, 0]
    for d in order:
        rows = pl.ds(other * 32 + xs[d] * 8, 8)
        pb[d] = sb[rows].astype(BF16)
        send(pb.at[d], r1b.at[d], ("c1b", d), sibling)
    arrived(r1a, ("c1a", 0))
    for d in range(1, NX):
        arrived(q2.at[y, :, from_x[d], c], ("p3b", d))
    for d in range(1, NY):
        send(q2.at[y, :, :, c], q2.at[y, :, :, c], ("p4b", d), at(y_=ys[d]))
    pair_a = sa[mine].reshape(NX, NZ, ROWS_A, LANES) + r1a[...].astype(F32)
    f2a[...] = pair_a
    s2a[...] = pair_a.astype(BF16)
    for d in range(1, NZ):
        send(s2a.at[:, zs[d]], r2a.at[d], ("c2a", d), at(z_=zs[d]))
    for d in order:
        arrived(r1b.at[d], ("c1b", d))
        rows = pl.ds(c * 32 + xs[d] * 8, 8)
        pair = sb[rows] + r1b[d].astype(F32)
        if d:
            s2b[d] = pair.astype(BF16)
            send(s2b.at[d], r2b.at[d], ("c2b", d), at(x_=xs[d]))
        else:
            t32b[...] = pair
    drain("low", "c1a", "c1b", "p2b", "p3b")
    for d in range(1, NX):
        arrived(r2b.at[d], ("c2b", d))
    column = t32b[...]
    for d in range(1, NX):
        column = column + r2b[d].astype(F32)
    t32b[...] = column
    t16b[...] = column.astype(BF16)
    for d in range(1, NZ):
        send(t16b.at[zs[d]], r3b.at[d], ("c3b", d), at(z_=zs[d]))
    for d in range(1, NZ):
        arrived(r2a.at[d], ("c2a", d))
    line = f2a[:, z]
    for d in range(1, NZ):
        line = line + r2a[d].astype(F32)
    t32a[...] = line
    t16a[...] = line.astype(BF16)
    for d in range(1, NX):
        send(t16a.at[xs[d]], r3a.at[d], ("c3a", d), at(x_=xs[d]))
    arrived(q1.at[1 - zh, x, c], ("p2a", 0))
    for d in range(1, NX):
        send(q1.at[1 - zh, x, c], q1.at[1 - zh, x, c], ("p3c", d), at(x_=xs[d]))
    send(q2.at[y, :, :, c], q2.at[y, :, :, c], ("p5b", 0), sibling)
    send(q1.at[:, x, c], q1.at[:, x, c], ("p5a", 0), sibling)
    for d in range(1, NX):
        arrived(q1.at[zh, from_x[d], c], ("p3a", d))
    scale = adapter_scale / ROLLOUT_TOKENS
    for d in range(1, NX):
        arrived(r3a.at[d], ("c3a", d))
    grad_a = t32a[x]
    for d in range(1, NX):
        grad_a = grad_a + r3a[d].astype(F32)
    grad_a = grad_a * scale
    new_a, _, _ = adam_update(fa[:, 0, :], ma[:, 0, :], va[:, 0, :], grad_a)
    for h in range(2):
        ez[h, z] = new_a[8 * h : 8 * h + 8].astype(BF16)
    for d in range(1, NZ):
        send(ez.at[:, z], ez.at[:, z], ("ez", d), at(z_=zs[d]))
    for d in range(1, NZ):
        arrived(r3b.at[d], ("c3b", d))
    grad_b = t32b[z]
    for d in range(1, NZ):
        grad_b = grad_b + r3b[d].astype(F32)
    grad_b = grad_b * scale
    grad_out[0:ROWS_A] = grad_a
    grad_out[ROWS_A:ROWS] = grad_b
    new_b, _, _ = adam_update(fb[:, 0, :], mb[:, 0, :], vb[:, 0, :], grad_b)
    blocks = jnp.concatenate(in_wide_blocks(new_b), axis=0).astype(BF16)
    for kk in range(4):
        ebz[z, kk] = blocks[8 * kk : 8 * kk + 8]
    y_zh, y_x = lax.div(y, 2), lax.rem(y, 2)
    on_way = zh == y_zh
    holder = zh * 2 + lax.div(x, 2)
    holds = y == holder

    def send_if(condition, src, dst, key, device):
        one = copy(src, dst, key, device)
        sent.append((key[0], condition, one))
        pl.when(condition)(one.start)

    def arrived_if(condition, dst, key):
        pl.when(condition)(lambda: arrived(dst, key))

    for d in range(1, NZ):
        send_if(lax.div(zs[d], 4) == y_zh, ebz.at[z], ebz.at[z], ("bz", d), at(z_=zs[d]))

    for d in range(1, NY):
        arrived(q2.at[from_y[d], :, :, c], ("p4b", d))
        send(q2.at[from_y[d], :, :, c], q2.at[from_y[d], :, :, c], ("p5b", d), sibling)
    drain("c2a", "c2b", "c3a", "c3b", "p2a", "p3a", "p4b")
    for d in range(1, NZ):
        arrived(ez.at[:, from_z[d]], ("ez", d))
    for d in range(1, NX):
        send(ez.at[0], ea0.at[x], ("ex", d), at(x_=xs[d]))
    for d in range(1, NY):
        send(ez.at[1], ea1.at[y], ("ey", d), at(y_=ys[d]))
    ea0[x] = ez[0]
    ea1[y] = ez[1]
    for d in range(1, NZ):
        arrived_if(on_way, ebz.at[from_z[d]], ("bz", d))

    def two_blocks(xx):
        return ebz.at[:, pl.ds(lax.rem(xx, 2) * 2, 2)]

    for d in range(1, NX):
        target = jnp.logical_and(on_way, lax.div(xs[d], 2) == y_x)
        send_if(target, two_blocks(xs[d]), ebx.at[x], ("bx", d), at(x_=xs[d]))

    for d in range(1, NX):
        arrived(q1.at[1 - zh, from_x[d], c], ("p3c", d))
        send(q1.at[:, from_x[d], c], q1.at[:, from_x[d], c], ("p5a", d), sibling)
    load_base.wait()
    for d in range(NY):
        arrived(q2.at[from_y[d], :, :, other], ("p5b", d))
    total = jnp.zeros((BLOCK, 256), F32)
    for yy in range(NY):
        columns = slice(HALF + yy * PART, HALF + (yy + 1) * PART)
        total = total + dot_nt(base[:, columns], q2[yy].reshape(256, PART))
    part_out[...] = total

    for d in range(1, NX):
        arrived(ea0.at[from_x[d]], ("ex", d))
    for xx in range(NX):
        stga[xx * NZ : (xx + 1) * NZ] = ea0[xx].astype(F32)
    for j in range(8):
        ha0[y, c, :, j * LANES : (j + 1) * LANES] = stga[:, j, :].astype(BF16)
    for d in range(1, NY):
        send(ha0.at[y, c], ha0.at[y, c], ("fy", d), at(y_=ys[d]))
    send(ha0.at[y, c], ha0.at[y, c], ("fc", 0), sibling)
    for d in range(1, NY):
        arrived(ea1.at[from_y[d]], ("ey", d))
    for yy in range(NY):
        stgy[yy] = ea1[yy].astype(F32)
    for yy in range(NY):
        for j in range(8):
            ha1[yy, c, x, :, j * LANES : (j + 1) * LANES] = stgy[yy, :, j, :].astype(BF16)
    for d in range(1, NX):
        send(ha1.at[:, c, x], ha1.at[:, c, x], ("fx", d), at(x_=xs[d]))
    send(ha1.at[:, c, x], ha1.at[:, c, x], ("fd", 0), sibling)

    @pl.when(holds)
    def _():
        ebx[x] = ebz[:, pl.ds(lax.rem(x, 2) * 2, 2)]
        for d in range(1, NX):
            arrived(ebx.at[from_x[d]], ("bx", d))

    send_if(holds, ebx.at[:, :, other], ebd, ("bc", 0), sibling)

    for d in range(NX):
        arrived(q1.at[:, from_x[d], other], ("p5a", d))
    part_out[...] = part_out[...] + dot_nt(base[:, 0:HALF], q1[...].reshape(256, HALF))
    @pl.when(holds)
    def _():
        for xx in range(NX):
            stgb[c, xx * NZ : (xx + 1) * NZ] = ebx[xx, :, c].astype(F32)
        arrived(ebd, ("bc", 0))
        for xx in range(NX):
            stgb[other, xx * NZ : (xx + 1) * NZ] = ebd[xx].astype(F32)
        for yy in range(NY):
            for cc in range(NC):
                for h in range(2):
                    bs[yy, cc, :, h * LANES : (h + 1) * LANES] = stgb[
                        cc, :, 2 * yy + h, :
                    ].astype(BF16)
        bb[...] = bs[y]

    for d in range(1, NY):
        send_if(holds, bs.at[ys[d]], bb, ("by", d), at(y_=ys[d]))

    drain("ez", "ex", "ey", "p3c", "p5a", "p5b", "bz", "bx")
    for d in range(1, NY):
        arrived(ha0.at[from_y[d], c], ("fy", d))
        send(ha0.at[from_y[d], c], ha0.at[from_y[d], c], ("fc", d), sibling)
    for d in range(1, NX):
        arrived(ha1.at[:, c, from_x[d]], ("fx", d))
        send(ha1.at[:, c, from_x[d]], ha1.at[:, c, from_x[d]], ("fd", d), sibling)
    for d in range(NY):
        arrived(ha0.at[from_y[d], other], ("fc", d))
    for d in range(NX):
        arrived(ha1.at[:, other, from_x[d]], ("fd", d))

    cross = jnp.zeros((RANK, 256), F32)
    for yy in range(NY):
        left = (
            ha0[yy].reshape(RANK, PART),
            ha1[yy].astype(F32).reshape(RANK, PART).astype(BF16),
        )
        for h in range(2):
            if yy < 2:
                first = (2 * yy + h) * PART
                right = q1[:, :, :, :, first : first + PART].reshape(256, PART)
            else:
                right = q2[2 * (yy - 2) + h].reshape(256, PART)
            cross = cross + dot_nt(left[h], right)
    high = cross.astype(BF16)
    low_part = (cross - high.astype(F32)).astype(BF16)

    for d in range(1, NY):
        arrived_if(from_y[d] == holder, bb, ("by", d))
    turned = bb[...].reshape(RANK, WIDE).astype(F32).T.astype(BF16)[0:BLOCK]
    adapter = dot_nn(turned, high) + dot_nn(turned, low_part)
    part_out[...] = part_out[...] + adapter_scale * adapter

    drain()


SEMAPHORES = 128


def in_hbm(array):
    return pltpu.with_memory_space_constraint(array, pltpu.HBM)


def exchange(act, cot, keep, fa, ma, va, fb, mb, vb, prompts, base):
    hbm = pl.BlockSpec(memory_space=pltpu.HBM)
    vmem = pl.BlockSpec(memory_space=pltpu.VMEM)
    smem = pl.BlockSpec(memory_space=pltpu.SMEM)
    tokens = act.shape[0]
    sds = jax.ShapeDtypeStruct
    tile_a, tile_b = (ROWS_A, LANES), (ROWS_B, LANES)
    return pl.pallas_call(
        exchange_kernel,
        out_shape=(
            sds((ROWS, LANES), F32),
            sds((NY, NC, 32, 1024), BF16),
            sds((NY, NC, NX, 8, 1024), BF16),
            sds((NC, 32, WIDE), BF16),
            sds((BLOCK, 256), F32),
        ),
        in_specs=[hbm, hbm, smem] + [hbm] * 8,
        out_specs=(vmem,) * 5,
        scratch_shapes=[
            pltpu.VMEM((2, NX, NC, 16, 4096), BF16),
            pltpu.VMEM((NY, 2, NX, NC, 16, 1024), BF16),
            pltpu.VMEM(base.shape, BF16),
            pltpu.VMEM(act.shape, BF16),
            pltpu.VMEM(cot.shape, BF16),
            pltpu.VMEM(fa.shape, F32),
            pltpu.VMEM(fa.shape, F32),
            pltpu.VMEM(fa.shape, F32),
            pltpu.VMEM(fb.shape, F32),
            pltpu.VMEM(fb.shape, F32),
            pltpu.VMEM(fb.shape, F32),
            pltpu.VMEM((NC, NX, NZ, *tile_a), BF16),
            pltpu.VMEM((NC, NX, NZ, *tile_b), BF16),
            pltpu.VMEM((32, *tile_a), F32),
            pltpu.VMEM((NZ, *tile_b), F32),
            pltpu.VMEM((NC, 32, ROWS_A * LANES), F32),
            pltpu.VMEM((NC * NX, NZ, ROWS_B * LANES), F32),
            pltpu.VMEM((NY, 2 * RANK, tokens), BF16),
            pltpu.VMEM((RANK, *tile_a), F32),
            pltpu.VMEM((RANK, *tile_b), F32),
            pltpu.VMEM((NX, NZ, *tile_a), BF16),
            pltpu.VMEM((NX, NZ, *tile_b), BF16),
            pltpu.VMEM((NX, NZ, *tile_a), BF16),
            pltpu.VMEM((NX, NZ, *tile_b), BF16),
            pltpu.VMEM((NX, NZ, *tile_a), F32),
            pltpu.VMEM((NX, NZ, *tile_a), BF16),
            pltpu.VMEM((NX, NZ, *tile_b), BF16),
            pltpu.VMEM((NZ, NX, *tile_a), BF16),
            pltpu.VMEM((NX, NZ, *tile_b), BF16),
            pltpu.VMEM((NX, *tile_a), F32),
            pltpu.VMEM((NZ, *tile_b), F32),
            pltpu.VMEM((NX, *tile_a), BF16),
            pltpu.VMEM((NZ, *tile_b), BF16),
            pltpu.VMEM((NX, *tile_a), BF16),
            pltpu.VMEM((NZ, *tile_b), BF16),
            pltpu.VMEM((2, NZ, 8, LANES), BF16),
            pltpu.VMEM((NX, NZ, 8, LANES), BF16),
            pltpu.VMEM((NY, NZ, 8, LANES), BF16),
            pltpu.VMEM((NX * NZ, 8, LANES), F32),
            pltpu.VMEM((NY, NZ, 8, LANES), F32),
            pltpu.VMEM((NZ, 4, 8, LANES), BF16),
            pltpu.VMEM((NX, NZ, 2, 8, LANES), BF16),
            pltpu.VMEM((NX, NZ, 8, LANES), BF16),
            pltpu.VMEM((NC, NX * NZ, 8, LANES), F32),
            pltpu.VMEM((NY, NC, 32, WIDE), BF16),
            pltpu.VMEM((NY, 4, 4096), BF16),
            pltpu.VMEM((NY, 4, 1024), BF16),
            pltpu.VMEM((16, 4096), F32),
            pltpu.VMEM((16, 1024), F32),
            pltpu.SemaphoreType.DMA((11,)),
            pltpu.SemaphoreType.DMA((SEMAPHORES,)),
            pltpu.SemaphoreType.DMA((SEMAPHORES,)),
        ],
        compiler_params=pltpu.CompilerParams(
            collective_id=0, has_side_effects=True, vmem_limit_bytes=40 * 1024 * 1024
        ),
        cost_estimate=pl.CostEstimate(
            flops=200_000_000_000, bytes_accessed=8_000_000, transcendentals=0
        ),
        name="exchange",
    )(
        in_hbm(act),
        in_hbm(cot),
        keep,
        *map(in_hbm, (fa, ma, va, fb, mb, vb)),
        in_hbm(prompts),
        in_hbm(base),
    )


def merge_kernel(
    base, ha0, ha1, bb, part, grad, fa, ma, va, fb, mb, vb, ua, ub, na, nb, sa, sb, merged, proj, bt
):
    i = pl.program_id(0)

    @pl.when(i == 0)
    def _():
        bt[...] = bb[...].reshape(RANK, WIDE).astype(F32).T.astype(BF16)
        ua[:, 0, :], na[:, 0, :], sa[:, 0, :] = adam_update(
            fa[:, 0, :], ma[:, 0, :], va[:, 0, :], grad[0:ROWS_A]
        )
        ub[:, 0, :], nb[:, 0, :], sb[:, 0, :] = adam_update(
            fb[:, 0, :], mb[:, 0, :], vb[:, 0, :], grad[ROWS_A:ROWS]
        )
        proj[...] = part[...].astype(BF16)

    turned = bt[0:BLOCK, :]
    left = ha0[0].reshape(RANK, 1024)
    right = ha1[0].astype(F32).reshape(RANK, 1024).astype(BF16)
    for h, columns in enumerate((left, right)):
        here = slice(h * 1024, (h + 1) * 1024)
        delta = dot_nn(turned, columns)
        merged[:, here] = (base[:, here].astype(F32) + adapter_scale * delta).astype(BF16)


def merge(base, ha0, ha1, bb, part, grad, fa, ma, va, fb, mb, vb):
    sds = jax.ShapeDtypeStruct

    def fixed(shape):
        return pl.BlockSpec(shape, lambda i: (0,) * len(shape))

    a_shape, b_shape = (ROWS_A, 1, LANES), (ROWS_B, 1, LANES)
    return pl.pallas_call(
        merge_kernel,
        grid=(NY,),
        out_shape=(
            sds(a_shape, F32),
            sds(b_shape, F32),
            sds(a_shape, F32),
            sds(b_shape, F32),
            sds(a_shape, F32),
            sds(b_shape, F32),
            sds(base.shape, BF16),
            sds((BLOCK, 256), BF16),
        ),
        in_specs=[
            pl.BlockSpec((BLOCK, 2048), lambda i: (0, i)),
            pl.BlockSpec((1, NC, 32, 1024), lambda i: (i, 0, 0, 0)),
            pl.BlockSpec((1, NC, NX, 8, 1024), lambda i: (i, 0, 0, 0, 0)),
            fixed((NC, 32, WIDE)),
            fixed((BLOCK, 256)),
            fixed((ROWS, LANES)),
        ]
        + [fixed(a_shape)] * 3
        + [fixed(b_shape)] * 3,
        out_specs=[
            fixed(a_shape),
            fixed(b_shape),
            fixed(a_shape),
            fixed(b_shape),
            fixed(a_shape),
            fixed(b_shape),
            pl.BlockSpec((BLOCK, 2048), lambda i: (0, i)),
            fixed((BLOCK, 256)),
        ],
        scratch_shapes=[pltpu.VMEM((WIDE, RANK), BF16)],
        compiler_params=pltpu.CompilerParams(
            dimension_semantics=("arbitrary",), vmem_limit_bytes=16 * 1024 * 1024
        ),
        name="merge",
    )(base, ha0, ha1, bb, part, grad, fa, ma, va, fb, mb, vb)


def body(
    activations,
    cotangent,
    block_keep,
    input_factor,
    input_mean,
    input_square,
    output_factor,
    output_mean,
    output_square,
    frozen_base_rows,
    prompts,
):
    fa, ma, va = (v.reshape(ROWS_A, 1, LANES) for v in (input_factor, input_mean, input_square))
    fb, mb, vb = (v.reshape(ROWS_B, 1, LANES) for v in (output_factor, output_mean, output_square))
    grad, ha0, ha1, bb, part = exchange(
        activations,
        cotangent,
        block_keep,
        fa,
        ma,
        va,
        fb,
        mb,
        vb,
        prompts,
        frozen_base_rows,
    )
    ua, ub, na, nb, sa, sb, merged, projected = merge(
        frozen_base_rows, ha0, ha1, bb, part, grad, fa, ma, va, fb, mb, vb
    )
    return (
        ua.reshape(1, -1),
        ub.reshape(1, -1),
        na.reshape(1, -1),
        nb.reshape(1, -1),
        sa.reshape(1, -1),
        sb.reshape(1, -1),
        merged,
        projected,
    )


def solution(mesh):
    row = P(("role", "dp"), "tp")
    placed = (
        row,
        row,
        P(("role", "dp")),
        row,
        row,
        row,
        row,
        row,
        row,
        P(("dp", "tp"), None),
        P(("role", "dp", "tp"), None),
    )
    return jax.shard_map(
        body,
        mesh=mesh,
        in_specs=placed,
        out_specs=(
            row,
            row,
            row,
            row,
            row,
            row,
            P(("dp", "tp"), None),
            P(("dp", "tp"), "role"),
        ),
        check_vma=False,
    )
```

```python
import jax
import jax.numpy as jnp
from jax import lax
from jax.experimental import pallas as pl
from jax.experimental.pallas import tpu as pltpu
from jax.sharding import PartitionSpec as P

ROLLOUT_TOKENS = 256
RANK = 64
LANES = 128
ROWS_A, ROWS_B = 16, 28
ROWS = ROWS_A + ROWS_B
NX, NY, NZ, NC = 4, 4, 8, 2
BLOCK = 224
WIDE = 256
HALF, PART = 4096, 1024

adapter_scale = 2.0
learn_rate = 0.004
beta_one = 0.9
beta_two = 0.95
epsilon = 1e-08
first_fix = 1.0 - 0.9**20
second_fix = 1.0 - 0.95**20

F32, BF16 = jnp.float32, jnp.bfloat16
MESH = pl.DeviceIdType.MESH


def adam_update(factor, moment, square, gradient):
    moment_new = beta_one * moment + (1.0 - beta_one) * gradient
    square_new = beta_two * square + (1.0 - beta_two) * gradient * gradient
    factor_new = factor - learn_rate * (moment_new / first_fix) / (
        jnp.sqrt(square_new / second_fix) + epsilon
    )
    return (factor_new, moment_new, square_new)


def dot_nn(a, b):
    return lax.dot_general(a, b, (((1,), (0,)), ((), ())), preferred_element_type=F32)


def dot_nt(a, b):
    return lax.dot_general(a, b, (((1,), (1,)), ((), ())), preferred_element_type=F32)


def in_wide_blocks(rows):
    lane = lax.broadcasted_iota(jnp.int32, (1, LANES), 1)
    rolled = {0: rows}
    for off in (32, 64, 96):
        rolled[off] = pltpu.roll(rows, LANES - off, 1)
    out = []
    for k in range(16):
        row, off = divmod(BLOCK * k, LANES)
        turned = rolled[off]
        for half in range(2):
            first = turned[row + half : row + half + 1]
            if off == 0:
                out.append(first)
                continue
            last = min(row + half + 1, ROWS_B - 1)
            second = turned[last : last + 1]
            out.append(jnp.where(lane < LANES - off, first, second))
    return out


def exchange_kernel(
    act_hbm,
    cot_hbm,
    keep_ref,
    fa_hbm,
    ma_hbm,
    va_hbm,
    fb_hbm,
    mb_hbm,
    vb_hbm,
    prompts_hbm,
    base_hbm,
    grad_out,
    ha0,
    ha1,
    bb,
    part_out,
    cross_out,
    q1,
    q2,
    base,
    act,
    cot,
    fa,
    ma,
    va,
    fb,
    mb,
    vb,
    ga,
    gb,
    stg32,
    stg8,
    wa,
    wb,
    low,
    sa,
    sb,
    pa,
    pb,
    r1a,
    r1b,
    f2a,
    s2a,
    s2b,
    r2a,
    r2b,
    t32a,
    t32b,
    t16a,
    t16b,
    r3a,
    r3b,
    ez,
    ea0,
    ea1,
    stga,
    stgy,
    ebz,
    ebx,
    ebd,
    stgb,
    bs,
    pr1,
    pr2,
    pf1,
    pf2,
    loc,
    ssem,
    rsem,
):
    z_lo = lax.axis_index("role")
    dp = lax.axis_index("dp")
    y = lax.axis_index("tp")
    c = lax.rem(dp, 2)
    x = lax.rem(lax.div(dp, 2), 4)
    zh = lax.div(dp, 8)
    z = zh * 4 + z_lo

    def at(x_=x, y_=y, z_=z, c_=c):
        return {
            "role": lax.rem(z_, 4),
            "dp": lax.div(z_, 4) * 8 + x_ * 2 + c_,
            "tp": y_,
        }

    def step(v, d, n):
        return lax.rem(v + d, n)

    other = 1 - c
    sibling = at(c_=other)
    xs = [step(x, d, NX) for d in range(NX)]
    ys = [step(y, d, NY) for d in range(NY)]
    zs = [step(z, d, NZ) for d in range(NZ)]
    from_x = [step(x, NX - d, NX) for d in range(NX)]
    from_y = [step(y, NY - d, NY) for d in range(NY)]
    from_z = [step(z, NZ - d, NZ) for d in range(NZ)]

    stages, free, leaving, whole = {}, list(range(SENDS))[::-1], {}, {}

    def copy(src, dst, stage, key, device):
        return pltpu.make_async_remote_copy(
            src_ref=src,
            dst_ref=dst,
            send_sem=ssem.at[leaving[key][0]],
            recv_sem=rsem.at[stages.setdefault(stage, len(stages))],
            device_id=device,
            device_id_type=MESH,
        )

    def send(src, dst, stage, device):
        if stage not in leaving:
            leaving[stage] = (free.pop(), None, None)
        copy(src, dst, stage, stage, device).start()

    def send_if(condition, src, dst, stage, d, device):
        index = free.pop()
        leaving[stage, d] = (index, None, None)
        one = copy(src, dst, stage, (stage, d), device)
        leaving[stage, d] = (index, condition, one)
        pl.when(condition)(one.start)

    def arrived(all_of_it, stage):
        whole[stage] = all_of_it
        semaphore = rsem.at[stages[stage]]
        pltpu.make_async_copy(all_of_it, all_of_it, semaphore).wait()

    def drain(*keys):
        for key in keys:
            index, condition, one = leaving.pop(key)
            if one is None:
                pltpu.make_async_copy(whole[key], whole[key], ssem.at[index]).wait()
            else:
                pl.when(condition)(one.wait_send)
            free.append(index)

    load_act = pltpu.make_async_copy(act_hbm, act, loc.at[0])
    load_cot = pltpu.make_async_copy(cot_hbm, cot, loc.at[1])
    loads = [
        pltpu.make_async_copy(src, dst, loc.at[3 + i])
        for i, (src, dst) in enumerate(
            ((fa_hbm, fa), (fb_hbm, fb), (ma_hbm, ma), (va_hbm, va), (mb_hbm, mb), (vb_hbm, vb))
        )
    ]
    for one in loads[:2]:
        one.start()

    def late(yy):
        return prompts_hbm.at[:, pl.ds(pl.multiple_of(HALF + yy * PART, PART), PART)]

    early = prompts_hbm.at[:, 0:HALF]
    load_early = pltpu.make_async_copy(early, pr1.at[y], loc.at[2])
    load_late = pltpu.make_async_copy(late(y), pr2.at[y], loc.at[9])
    load_base = pltpu.make_async_copy(base_hbm, base, loc.at[10])
    load_early.start()
    load_late.start()
    load_act.start()
    load_cot.start()
    for one in loads[2:]:
        one.start()
    load_base.start()

    barrier = pltpu.get_barrier_semaphore()
    peers = (
        [sibling]
        + [at(x_=v) for v in xs[1:]]
        + [at(y_=v) for v in ys[1:]]
        + [at(z_=v) for v in zs[1:]]
    )
    for peer in peers:
        pl.semaphore_signal(barrier, inc=1, device_id=peer, device_id_type=MESH)

    for one in loads[:2]:
        one.wait()
    ga[c, x, z] = fa[:, 0, :].astype(BF16)
    gb[c, x, z] = fb[:, 0, :].astype(BF16)
    pl.semaphore_wait(barrier, len(peers))

    for d in range(1, NX):
        send(ga.at[c, x, z], ga.at[c, x, z], "gax", at(x_=xs[d]))
    for d in range(1, NZ):
        send(gb.at[c, x, z], gb.at[c, x, z], "gbz", at(z_=zs[d]))
    for d in range(1, NY):
        send(late(ys[d]), pr2.at[y], "p1b", at(y_=ys[d]))
    for d in range(1, NY):
        send(early, pr1.at[y], "p1a", at(y_=ys[d]))
    arrived(ga.at[c, 0 : NX - 1, z], "gax")
    for d in range(1, NZ):
        send(ga.at[c, :, z], ga.at[c, :, z], "gaz", at(z_=zs[d]))
    arrived(gb.at[c, x, 0 : NZ - 1], "gbz")
    for d in range(1, NX):
        send(gb.at[c, x], gb.at[c, x], "gbx", at(x_=xs[d]))
    send(gb.at[c, x], gb.at[c, x], "gbc", sibling)

    def spread_a(core):
        stg32[...] = ga[core].reshape(32, ROWS_A, LANES).astype(F32)
        for j in range(ROWS_A):
            wa[core, :, j * LANES : (j + 1) * LANES] = stg32[:, j, :]

    def spread_b(core, xx):
        stg8[...] = gb[core, xx].astype(F32)
        for j in range(ROWS_B):
            wb[core * 4 + xx, :, j * LANES : (j + 1) * LANES] = stg8[:, j, :]

    spread_b(c, x)

    z_pair = at(z_=step(z, 4, NZ))
    load_late.wait()
    arrived(pr2.at[0 : NY - 1], "p1b")
    for yy in range(NY):
        pf2[4 * yy : 4 * yy + 4, :] = pr2[yy].astype(F32)
    q2[y, zh, x, c] = pf2[...].astype(BF16)
    load_early.wait()
    arrived(pr1.at[0 : NY - 1], "p1a")
    for yy in range(NY):
        pf1[4 * yy : 4 * yy + 4, :] = pr1[yy].astype(F32)
    q1[zh, x, c] = pf1[...].astype(BF16)

    arrived(ga.at[c, :, 0 : NZ - 1], "gaz")
    send(ga.at[c], ga.at[c], "gac", sibling)
    send(q2.at[y, zh, x, c], q2.at[y, zh, x, c], "p2b", z_pair)
    spread_a(c)
    arrived(gb.at[c, 0 : NX - 1], "gbx")
    for d in range(1, NX):
        send(gb.at[c, from_x[d]], gb.at[c, from_x[d]], "gbc", sibling)
        spread_b(c, from_x[d])
    for d in range(1, NX):
        send(q1.at[zh, x, c], q1.at[zh, x, c], "p3a", at(x_=xs[d]))
    arrived(ga.at[other], "gac")
    send(q1.at[zh, x, c], q1.at[zh, x, c], "p2a", z_pair)
    spread_a(other)
    arrived(gb.at[other], "gbc")
    for d in range(NX):
        spread_b(other, from_x[d])

    load_act.wait()
    load_cot.wait()
    for one in loads[2:]:
        one.wait()
    wide_a = wa[...].reshape(RANK, ROWS_A * LANES).astype(BF16)
    wide_b = wb[...].reshape(RANK, ROWS_B * LANES).astype(BF16)
    low[y, :, 0:RANK] = dot_nt(act[...], wide_a).astype(BF16)
    low[y, :, RANK : 2 * RANK] = dot_nt(cot[...], wide_b).astype(BF16)
    for d in range(1, NY):
        send(low.at[y], low.at[y], "low", at(y_=ys[d]))
    arrived(q2.at[y, 1 - zh, x, c], "p2b")
    for d in range(1, NX):
        send(q2.at[y, :, x, c], q2.at[y, :, x, c], "p3b", at(x_=xs[d]))
    drain("gax", "gaz", "gac", "gbz", "gbx", "gbc", "p1a", "p1b")
    arrived(low.at[0 : NY - 1], "low")
    total = low[0].astype(F32)
    for yy in range(1, NY):
        total = total + low[yy].astype(F32)
    kept = (total * keep_ref[0].astype(F32)).T.astype(BF16)
    input_kept, grad_kept = kept[0:RANK], kept[RANK : 2 * RANK]

    chunk = 4
    for first in range(0, ROWS_A, chunk):
        part = dot_nn(grad_kept, act[:, first * LANES : (first + chunk) * LANES])
        for j in range(chunk):
            sa[:, first + j, :] = part[:, j * LANES : (j + 1) * LANES]
    mine, theirs = pl.ds(c * 32, 32), pl.ds(other * 32, 32)
    pa[...] = sa[theirs].reshape(NX, NZ, ROWS_A, LANES).astype(BF16)
    send(pa, r1a, "c1a", sibling)
    for first in range(0, ROWS_B, chunk):
        part = dot_nn(input_kept, cot[:, first * LANES : (first + chunk) * LANES])
        for j in range(chunk):
            sb[:, first + j, :] = part[:, j * LANES : (j + 1) * LANES]

    order = [1, 2, 3, 0]
    for d in order:
        rows = pl.ds(other * 32 + xs[d] * 8, 8)
        pb[d] = sb[rows].astype(BF16)
        send(pb.at[d], r1b.at[d], f"c1b{d}", sibling)
    arrived(r1a, "c1a")
    pair_a = sa[mine].reshape(NX, NZ, ROWS_A, LANES) + r1a[...].astype(F32)
    f2a[...] = pair_a
    s2a[...] = pair_a.astype(BF16)
    for d in range(1, NZ):
        send(s2a.at[:, zs[d]], r2a.at[d], "c2a", at(z_=zs[d]))
    for d in order:
        arrived(r1b.at[d], f"c1b{d}")
        rows = pl.ds(c * 32 + xs[d] * 8, 8)
        pair = sb[rows] + r1b[d].astype(F32)
        if d:
            s2b[d] = pair.astype(BF16)
            send(s2b.at[d], r2b.at[d], "c2b", at(x_=xs[d]))
        else:
            t32b[...] = pair
    arrived(q2.at[y, :, 0 : NX - 1, c], "p3b")
    for d in range(1, NY):
        send(q2.at[y, :, :, c], q2.at[y, :, :, c], "p4b", at(y_=ys[d]))
    drain("low", "c1a", *(f"c1b{d}" for d in order), "p2b")
    arrived(r2b.at[1:NX], "c2b")
    column = t32b[...]
    for d in range(1, NX):
        column = column + r2b[d].astype(F32)
    t32b[...] = column
    t16b[...] = column.astype(BF16)
    for d in range(1, NZ):
        send(t16b.at[zs[d]], r3b.at[d], "c3b", at(z_=zs[d]))
    arrived(r2a.at[1:NZ], "c2a")
    line = f2a[:, z]
    for d in range(1, NZ):
        line = line + r2a[d].astype(F32)
    t32a[...] = line
    t16a[...] = line.astype(BF16)
    for d in range(1, NX):
        send(t16a.at[xs[d]], r3a.at[d], "c3a", at(x_=xs[d]))
    arrived(q1.at[1 - zh, x, c], "p2a")
    for d in range(1, NX):
        send(q1.at[1 - zh, x, c], q1.at[1 - zh, x, c], "p3c", at(x_=xs[d]))
    send(q2.at[y, :, :, c], q2.at[y, :, :, c], "p5b", sibling)
    send(q1.at[:, x, c], q1.at[:, x, c], "p5a", sibling)
    arrived(q1.at[0, 0 : NX - 1, c], "p3a")
    scale = adapter_scale / ROLLOUT_TOKENS
    arrived(r3a.at[1:NX], "c3a")
    grad_a = t32a[x]
    for d in range(1, NX):
        grad_a = grad_a + r3a[d].astype(F32)
    grad_a = grad_a * scale
    new_a, _, _ = adam_update(fa[:, 0, :], ma[:, 0, :], va[:, 0, :], grad_a)
    for h in range(2):
        ez[h, z] = new_a[8 * h : 8 * h + 8].astype(BF16)
    for d in range(1, NZ):
        send(ez.at[:, z], ez.at[:, z], "ez", at(z_=zs[d]))
    arrived(r3b.at[1:NZ], "c3b")
    grad_b = t32b[z]
    for d in range(1, NZ):
        grad_b = grad_b + r3b[d].astype(F32)
    grad_b = grad_b * scale
    grad_out[0:ROWS_A] = grad_a
    grad_out[ROWS_A:ROWS] = grad_b
    new_b, _, _ = adam_update(fb[:, 0, :], mb[:, 0, :], vb[:, 0, :], grad_b)
    blocks = jnp.concatenate(in_wide_blocks(new_b), axis=0).astype(BF16)
    for kk in range(4):
        ebz[z, kk] = blocks[8 * kk : 8 * kk + 8]
    y_zh, y_x = lax.div(y, 2), lax.rem(y, 2)
    on_way = zh == y_zh
    holder = zh * 2 + lax.div(x, 2)
    holds = y == holder

    def arrived_if(condition, dst, stage):
        pl.when(condition)(lambda: arrived(dst, stage))

    for d in range(1, NZ):
        send_if(lax.div(zs[d], 4) == y_zh, ebz.at[z], ebz.at[z], "bz", d, at(z_=zs[d]))

    drain("c2a", "c2b", "c3a", "c3b", "p2a", "p3a", "p3b")
    arrived(ez.at[:, 0 : NZ - 1], "ez")
    for d in range(1, NX):
        send(ez.at[0], ea0.at[x], "ex", at(x_=xs[d]))
    for d in range(1, NY):
        send(ez.at[1], ea1.at[y], "ey", at(y_=ys[d]))
    ea0[x] = ez[0]
    ea1[y] = ez[1]
    arrived_if(on_way, ebz.at[0 : NZ - 1], "bz")

    def two_blocks(xx):
        return ebz.at[:, pl.ds(lax.rem(xx, 2) * 2, 2)]

    for d in range(1, NX):
        target = jnp.logical_and(on_way, lax.div(xs[d], 2) == y_x)
        send_if(target, two_blocks(xs[d]), ebx.at[x], "bx", d, at(x_=xs[d]))

    arrived(q2.at[0 : NY - 1, :, :, c], "p4b")
    for d in range(1, NY):
        send(q2.at[from_y[d], :, :, c], q2.at[from_y[d], :, :, c], "p5b", sibling)
    arrived(q1.at[0, 0 : NX - 1, c], "p3c")
    for d in range(1, NX):
        send(q1.at[:, from_x[d], c], q1.at[:, from_x[d], c], "p5a", sibling)
    arrived(ea0.at[0 : NX - 1], "ex")
    for xx in range(NX):
        stga[xx * NZ : (xx + 1) * NZ] = ea0[xx].astype(F32)
    for j in range(8):
        ha0[y, c, :, j * LANES : (j + 1) * LANES] = stga[:, j, :].astype(BF16)
    for d in range(1, NY):
        send(ha0.at[y, c], ha0.at[y, c], "fy", at(y_=ys[d]))
    send(ha0.at[y, c], ha0.at[y, c], "fc", sibling)
    arrived(ea1.at[0 : NY - 1], "ey")
    for yy in range(NY):
        stgy[yy] = ea1[yy].astype(F32)
    for yy in range(NY):
        for j in range(8):
            ha1[yy, c, x, :, j * LANES : (j + 1) * LANES] = stgy[yy, :, j, :].astype(BF16)
    for d in range(1, NX):
        send(ha1.at[:, c, x], ha1.at[:, c, x], "fx", at(x_=xs[d]))
    send(ha1.at[:, c, x], ha1.at[:, c, x], "fd", sibling)

    @pl.when(holds)
    def _():
        ebx[x] = ebz[:, pl.ds(lax.rem(x, 2) * 2, 2)]
        arrived(ebx.at[0 : NX - 1], "bx")

    send_if(holds, ebx.at[:, :, other], ebd, "bc", 0, sibling)

    load_base.wait()
    arrived(q2.at[:, :, :, other], "p5b")
    total = jnp.zeros((BLOCK, 256), F32)
    for yy in range(NY):
        columns = slice(HALF + yy * PART, HALF + (yy + 1) * PART)
        total = total + dot_nt(base[:, columns], q2[yy].reshape(256, PART))
    part_out[...] = total

    @pl.when(holds)
    def _():
        for xx in range(NX):
            stgb[c, xx * NZ : (xx + 1) * NZ] = ebx[xx, :, c].astype(F32)
        arrived(ebd, "bc")
        for xx in range(NX):
            stgb[other, xx * NZ : (xx + 1) * NZ] = ebd[xx].astype(F32)
        for yy in range(NY):
            for cc in range(NC):
                for h in range(2):
                    bs[yy, cc, :, h * LANES : (h + 1) * LANES] = stgb[
                        cc, :, 2 * yy + h, :
                    ].astype(BF16)
        bb[...] = bs[y]

    for d in range(1, NY):
        send_if(holds, bs.at[ys[d]], bb, "by", d, at(y_=ys[d]))

    arrived(q1.at[:, :, other], "p5a")
    part_out[...] = part_out[...] + dot_nt(base[:, 0:HALF], q1[...].reshape(256, HALF))
    drain("ez", "ex", "ey", "p3c", "p4b", "p5a", "p5b", *((k, d) for k, n in (("bz", NZ), ("bx", NX)) for d in range(1, n)))
    arrived(ha0.at[0 : NY - 1, c], "fy")
    for d in range(1, NY):
        send(ha0.at[from_y[d], c], ha0.at[from_y[d], c], "fc", sibling)
    arrived(ha1.at[:, c, 0 : NX - 1], "fx")
    for d in range(1, NX):
        send(ha1.at[:, c, from_x[d]], ha1.at[:, c, from_x[d]], "fd", sibling)
    arrived(ha0.at[:, other], "fc")
    arrived(ha1.at[:, other], "fd")

    cross = jnp.zeros((256, RANK), F32)
    for yy in range(NY):
        left = (
            ha0[yy].reshape(RANK, PART),
            ha1[yy].astype(F32).reshape(RANK, PART).astype(BF16),
        )
        for h in range(2):
            if yy < 2:
                first = (2 * yy + h) * PART
                right = q1[:, :, :, :, first : first + PART].reshape(256, PART)
            else:
                right = q2[2 * (yy - 2) + h].reshape(256, PART)
            cross = cross + dot_nt(right, left[h])
    high = cross.astype(BF16)
    cross_out[:, 0:RANK] = high
    cross_out[:, RANK : 2 * RANK] = (cross - high.astype(F32)).astype(BF16)

    arrived_if(y != holder, bb, "by")
    drain(*leaving)


ARRIVALS, SENDS = 37, 26


def in_hbm(array):
    return pltpu.with_memory_space_constraint(array, pltpu.HBM)


def exchange(act, cot, keep, fa, ma, va, fb, mb, vb, prompts, base):
    hbm = pl.BlockSpec(memory_space=pltpu.HBM)
    vmem = pl.BlockSpec(memory_space=pltpu.VMEM)
    smem = pl.BlockSpec(memory_space=pltpu.SMEM)
    tokens = act.shape[0]
    sds = jax.ShapeDtypeStruct
    tile_a, tile_b = (ROWS_A, LANES), (ROWS_B, LANES)
    return pl.pallas_call(
        exchange_kernel,
        out_shape=(
            sds((ROWS, LANES), F32),
            sds((NY, NC, 32, 1024), BF16),
            sds((NY, NC, NX, 8, 1024), BF16),
            sds((NC, 32, WIDE), BF16),
            sds((BLOCK, 256), F32),
            sds((256, 2 * RANK), BF16),
        ),
        in_specs=[hbm, hbm, smem] + [hbm] * 8,
        out_specs=(vmem,) * 6,
        scratch_shapes=[
            pltpu.VMEM((2, NX, NC, 16, 4096), BF16),
            pltpu.VMEM((NY, 2, NX, NC, 16, 1024), BF16),
            pltpu.VMEM(base.shape, BF16),
            pltpu.VMEM(act.shape, BF16),
            pltpu.VMEM(cot.shape, BF16),
            pltpu.VMEM(fa.shape, F32),
            pltpu.VMEM(fa.shape, F32),
            pltpu.VMEM(fa.shape, F32),
            pltpu.VMEM(fb.shape, F32),
            pltpu.VMEM(fb.shape, F32),
            pltpu.VMEM(fb.shape, F32),
            pltpu.VMEM((NC, NX, NZ, *tile_a), BF16),
            pltpu.VMEM((NC, NX, NZ, *tile_b), BF16),
            pltpu.VMEM((32, *tile_a), F32),
            pltpu.VMEM((NZ, *tile_b), F32),
            pltpu.VMEM((NC, 32, ROWS_A * LANES), F32),
            pltpu.VMEM((NC * NX, NZ, ROWS_B * LANES), F32),
            pltpu.VMEM((NY, tokens, 2 * RANK), BF16),
            pltpu.VMEM((RANK, *tile_a), F32),
            pltpu.VMEM((RANK, *tile_b), F32),
            pltpu.VMEM((NX, NZ, *tile_a), BF16),
            pltpu.VMEM((NX, NZ, *tile_b), BF16),
            pltpu.VMEM((NX, NZ, *tile_a), BF16),
            pltpu.VMEM((NX, NZ, *tile_b), BF16),
            pltpu.VMEM((NX, NZ, *tile_a), F32),
            pltpu.VMEM((NX, NZ, *tile_a), BF16),
            pltpu.VMEM((NX, NZ, *tile_b), BF16),
            pltpu.VMEM((NZ, NX, *tile_a), BF16),
            pltpu.VMEM((NX, NZ, *tile_b), BF16),
            pltpu.VMEM((NX, *tile_a), F32),
            pltpu.VMEM((NZ, *tile_b), F32),
            pltpu.VMEM((NX, *tile_a), BF16),
            pltpu.VMEM((NZ, *tile_b), BF16),
            pltpu.VMEM((NX, *tile_a), BF16),
            pltpu.VMEM((NZ, *tile_b), BF16),
            pltpu.VMEM((2, NZ, 8, LANES), BF16),
            pltpu.VMEM((NX, NZ, 8, LANES), BF16),
            pltpu.VMEM((NY, NZ, 8, LANES), BF16),
            pltpu.VMEM((NX * NZ, 8, LANES), F32),
            pltpu.VMEM((NY, NZ, 8, LANES), F32),
            pltpu.VMEM((NZ, 4, 8, LANES), BF16),
            pltpu.VMEM((NX, NZ, 2, 8, LANES), BF16),
            pltpu.VMEM((NX, NZ, 8, LANES), BF16),
            pltpu.VMEM((NC, NX * NZ, 8, LANES), F32),
            pltpu.VMEM((NY, NC, 32, WIDE), BF16),
            pltpu.VMEM((NY, 4, 4096), BF16),
            pltpu.VMEM((NY, 4, 1024), BF16),
            pltpu.VMEM((16, 4096), F32),
            pltpu.VMEM((16, 1024), F32),
            pltpu.SemaphoreType.DMA((11,)),
            pltpu.SemaphoreType.DMA((SENDS,)),
            pltpu.SemaphoreType.DMA((ARRIVALS,)),
        ],
        compiler_params=pltpu.CompilerParams(
            collective_id=0, has_side_effects=True, vmem_limit_bytes=40 * 1024 * 1024
        ),
        cost_estimate=pl.CostEstimate(
            flops=200_000_000_000, bytes_accessed=8_000_000, transcendentals=0
        ),
        name="exchange",
    )(
        in_hbm(act),
        in_hbm(cot),
        keep,
        *map(in_hbm, (fa, ma, va, fb, mb, vb)),
        in_hbm(prompts),
        in_hbm(base),
    )


def merge_kernel(
    base,
    ha0,
    ha1,
    bb,
    part,
    cross,
    grad,
    fa,
    ma,
    va,
    fb,
    mb,
    vb,
    ua,
    ub,
    na,
    nb,
    sa,
    sb,
    merged,
    proj,
    rows,
    done,
):
    turned = bb[...].reshape(RANK, WIDE).astype(F32).T.astype(BF16)[0:BLOCK]
    copies = []
    for yy in range(NY):
        left = ha0[yy].reshape(RANK, PART)
        right = ha1[yy].astype(F32).reshape(RANK, PART).astype(BF16)
        for h, columns in enumerate((left, right)):
            first = (2 * yy + h) * PART
            here = slice(first, first + PART)
            delta = dot_nn(turned, columns)
            rows[:, here] = (base[:, here].astype(F32) + adapter_scale * delta).astype(BF16)
            one = pltpu.make_async_copy(rows.at[:, here], merged.at[:, here], done.at[2 * yy + h])
            one.start()
            copies.append(one)
    ua[:, 0, :], na[:, 0, :], sa[:, 0, :] = adam_update(
        fa[:, 0, :], ma[:, 0, :], va[:, 0, :], grad[0:ROWS_A]
    )
    ub[:, 0, :], nb[:, 0, :], sb[:, 0, :] = adam_update(
        fb[:, 0, :], mb[:, 0, :], vb[:, 0, :], grad[ROWS_A:ROWS]
    )
    twice = jnp.concatenate([turned, turned], axis=1)
    proj[...] = (part[...] + adapter_scale * dot_nt(twice, cross[...])).astype(BF16)
    for one in copies:
        one.wait()


def merge(base, ha0, ha1, bb, part, cross, grad, fa, ma, va, fb, mb, vb):
    sds = jax.ShapeDtypeStruct
    vmem = pl.BlockSpec(memory_space=pltpu.VMEM)
    a_shape, b_shape = (ROWS_A, 1, LANES), (ROWS_B, 1, LANES)
    return pl.pallas_call(
        merge_kernel,
        out_shape=(
            sds(a_shape, F32),
            sds(b_shape, F32),
            sds(a_shape, F32),
            sds(b_shape, F32),
            sds(a_shape, F32),
            sds(b_shape, F32),
            sds(base.shape, BF16),
            sds((BLOCK, 256), BF16),
        ),
        in_specs=[vmem] * 13,
        out_specs=(vmem,) * 6 + (pl.BlockSpec(memory_space=pltpu.HBM), vmem),
        scratch_shapes=[pltpu.VMEM(base.shape, BF16), pltpu.SemaphoreType.DMA((2 * NY,))],
        compiler_params=pltpu.CompilerParams(vmem_limit_bytes=16 * 1024 * 1024),
        name="merge",
    )(base, ha0, ha1, bb, part, cross, grad, fa, ma, va, fb, mb, vb)


def body(
    activations,
    cotangent,
    block_keep,
    input_factor,
    input_mean,
    input_square,
    output_factor,
    output_mean,
    output_square,
    frozen_base_rows,
    prompts,
):
    fa, ma, va = (v.reshape(ROWS_A, 1, LANES) for v in (input_factor, input_mean, input_square))
    fb, mb, vb = (v.reshape(ROWS_B, 1, LANES) for v in (output_factor, output_mean, output_square))
    grad, ha0, ha1, bb, part, cross = exchange(
        activations,
        cotangent,
        block_keep,
        fa,
        ma,
        va,
        fb,
        mb,
        vb,
        prompts,
        frozen_base_rows,
    )
    ua, ub, na, nb, sa, sb, merged, projected = merge(
        frozen_base_rows, ha0, ha1, bb, part, cross, grad, fa, ma, va, fb, mb, vb
    )
    return (
        ua.reshape(1, -1),
        ub.reshape(1, -1),
        na.reshape(1, -1),
        nb.reshape(1, -1),
        sa.reshape(1, -1),
        sb.reshape(1, -1),
        merged,
        projected,
    )


def solution(mesh):
    row = P(("role", "dp"), "tp")
    placed = (
        row,
        row,
        P(("role", "dp")),
        row,
        row,
        row,
        row,
        row,
        row,
        P(("dp", "tp"), None),
        P(("role", "dp", "tp"), None),
    )
    return jax.shard_map(
        body,
        mesh=mesh,
        in_specs=placed,
        out_specs=(
            row,
            row,
            row,
            row,
            row,
            row,
            P(("dp", "tp"), None),
            P(("dp", "tp"), "role"),
        ),
        check_vma=False,
    )
```

```python
import jax
import jax.numpy as jnp
from jax import lax
from jax.experimental import pallas as pl
from jax.experimental.pallas import tpu as pltpu
from jax.sharding import PartitionSpec as P

ROLLOUT_TOKENS = 256
RANK = 64
LANES = 128
ROWS_A, ROWS_B = 16, 28
ROWS = ROWS_A + ROWS_B
NX, NY, NZ, NC = 4, 4, 8, 2
BLOCK = 224
WIDE = 256
HALF, PART = 4096, 1024

adapter_scale = 2.0
learn_rate = 0.004
beta_one = 0.9
beta_two = 0.95
epsilon = 1e-08
first_fix = 1.0 - 0.9**20
second_fix = 1.0 - 0.95**20

F32, BF16 = jnp.float32, jnp.bfloat16
MESH = pl.DeviceIdType.MESH


def adam_update(factor, moment, square, gradient):
    moment_new = beta_one * moment + (1.0 - beta_one) * gradient
    square_new = beta_two * square + (1.0 - beta_two) * gradient * gradient
    factor_new = factor - learn_rate * (moment_new / first_fix) / (
        jnp.sqrt(square_new / second_fix) + epsilon
    )
    return (factor_new, moment_new, square_new)


def dot_nn(a, b):
    return lax.dot_general(a, b, (((1,), (0,)), ((), ())), preferred_element_type=F32)


def dot_nt(a, b):
    return lax.dot_general(a, b, (((1,), (1,)), ((), ())), preferred_element_type=F32)


def in_wide_blocks(rows):
    lane = lax.broadcasted_iota(jnp.int32, (1, LANES), 1)
    rolled = {0: rows}
    for off in (32, 64, 96):
        rolled[off] = pltpu.roll(rows, LANES - off, 1)
    out = []
    for k in range(16):
        row, off = divmod(BLOCK * k, LANES)
        turned = rolled[off]
        for half in range(2):
            first = turned[row + half : row + half + 1]
            if off == 0:
                out.append(first)
                continue
            last = min(row + half + 1, ROWS_B - 1)
            second = turned[last : last + 1]
            out.append(jnp.where(lane < LANES - off, first, second))
    return out


def exchange_kernel(
    act_hbm,
    cot_hbm,
    keep_ref,
    fa_hbm,
    ma_hbm,
    va_hbm,
    fb_hbm,
    mb_hbm,
    vb_hbm,
    prompts_hbm,
    base_hbm,
    grad_out,
    ha0,
    ha1,
    bb,
    part_out,
    q1,
    q2,
    base,
    act,
    cot,
    fa,
    ma,
    va,
    fb,
    mb,
    vb,
    ga,
    gb,
    stg32,
    stg8,
    wa,
    wb,
    low,
    sa,
    sb,
    pa,
    pb,
    r1a,
    r1b,
    f2a,
    s2a,
    s2b,
    r2a,
    r2b,
    t32a,
    t32b,
    t16a,
    t16b,
    r3a,
    r3b,
    ez,
    ea0,
    ea1,
    stga,
    stgy,
    ebz,
    ebx,
    ebd,
    stgb,
    bs,
    pr1,
    pr2,
    pf1,
    pf2,
    loc,
    ssem,
    rsem,
):
    z_lo = lax.axis_index("role")
    dp = lax.axis_index("dp")
    y = lax.axis_index("tp")
    c = lax.rem(dp, 2)
    x = lax.rem(lax.div(dp, 2), 4)
    zh = lax.div(dp, 8)
    z = zh * 4 + z_lo

    def at(x_=x, y_=y, z_=z, c_=c):
        return {
            "role": lax.rem(z_, 4),
            "dp": lax.div(z_, 4) * 8 + x_ * 2 + c_,
            "tp": y_,
        }

    def step(v, d, n):
        return lax.rem(v + d, n)

    other = 1 - c
    sibling = at(c_=other)
    xs = [step(x, d, NX) for d in range(NX)]
    ys = [step(y, d, NY) for d in range(NY)]
    zs = [step(z, d, NZ) for d in range(NZ)]
    from_x = [step(x, NX - d, NX) for d in range(NX)]
    from_y = [step(y, NY - d, NY) for d in range(NY)]
    from_z = [step(z, NZ - d, NZ) for d in range(NZ)]

    stages, free, leaving, whole = {}, list(range(SENDS))[::-1], {}, {}

    def copy(src, dst, stage, key, device):
        return pltpu.make_async_remote_copy(
            src_ref=src,
            dst_ref=dst,
            send_sem=ssem.at[leaving[key][0]],
            recv_sem=rsem.at[stages.setdefault(stage, len(stages))],
            device_id=device,
            device_id_type=MESH,
        )

    def send(src, dst, stage, device):
        if stage not in leaving:
            leaving[stage] = (free.pop(), None, None)
        copy(src, dst, stage, stage, device).start()

    def send_if(condition, src, dst, stage, d, device):
        index = free.pop()
        leaving[stage, d] = (index, None, None)
        one = copy(src, dst, stage, (stage, d), device)
        leaving[stage, d] = (index, condition, one)
        pl.when(condition)(one.start)

    def arrived(all_of_it, stage):
        whole[stage] = all_of_it
        semaphore = rsem.at[stages[stage]]
        pltpu.make_async_copy(all_of_it, all_of_it, semaphore).wait()

    def drain(*keys):
        for key in keys:
            index, condition, one = leaving.pop(key)
            if one is None:
                pltpu.make_async_copy(whole[key], whole[key], ssem.at[index]).wait()
            else:
                pl.when(condition)(one.wait_send)
            free.append(index)

    load_act = pltpu.make_async_copy(act_hbm, act, loc.at[0])
    load_cot = pltpu.make_async_copy(cot_hbm, cot, loc.at[1])
    loads = [
        pltpu.make_async_copy(src, dst, loc.at[3 + i])
        for i, (src, dst) in enumerate(
            ((fa_hbm, fa), (fb_hbm, fb), (ma_hbm, ma), (va_hbm, va), (mb_hbm, mb), (vb_hbm, vb))
        )
    ]
    for one in loads[:2]:
        one.start()

    def late(yy):
        return prompts_hbm.at[:, pl.ds(pl.multiple_of(HALF + yy * PART, PART), PART)]

    early = prompts_hbm.at[:, 0:HALF]
    load_early = pltpu.make_async_copy(early, pr1.at[y], loc.at[2])
    load_late = pltpu.make_async_copy(late(y), pr2.at[y], loc.at[9])
    load_base = pltpu.make_async_copy(base_hbm, base, loc.at[10])
    load_early.start()
    load_late.start()
    load_act.start()
    load_cot.start()
    for one in loads[2:]:
        one.start()
    load_base.start()

    barrier = pltpu.get_barrier_semaphore()
    peers = (
        [sibling]
        + [at(x_=v) for v in xs[1:]]
        + [at(y_=v) for v in ys[1:]]
        + [at(z_=v) for v in zs[1:]]
    )
    for peer in peers:
        pl.semaphore_signal(barrier, inc=1, device_id=peer, device_id_type=MESH)

    for one in loads[:2]:
        one.wait()
    ga[c, x, z] = fa[:, 0, :].astype(BF16)
    gb[c, x, z] = fb[:, 0, :].astype(BF16)
    pl.semaphore_wait(barrier, len(peers))

    for d in range(1, NX):
        send(ga.at[c, x, z], ga.at[c, x, z], "gax", at(x_=xs[d]))
    for d in range(1, NZ):
        send(gb.at[c, x, z], gb.at[c, x, z], "gbz", at(z_=zs[d]))
    for d in range(1, NY):
        send(late(ys[d]), pr2.at[y], "p1b", at(y_=ys[d]))
    for d in range(1, NY):
        send(early, pr1.at[y], "p1a", at(y_=ys[d]))
    arrived(ga.at[c, 0 : NX - 1, z], "gax")
    for d in range(1, NZ):
        send(ga.at[c, :, z], ga.at[c, :, z], "gaz", at(z_=zs[d]))
    arrived(gb.at[c, x, 0 : NZ - 1], "gbz")
    for d in range(1, NX):
        send(gb.at[c, x], gb.at[c, x], "gbx", at(x_=xs[d]))
    send(gb.at[c, x], gb.at[c, x], "gbc", sibling)

    def spread_a(core):
        stg32[...] = ga[core].reshape(32, ROWS_A, LANES).astype(F32)
        for j in range(ROWS_A):
            wa[core, :, j * LANES : (j + 1) * LANES] = stg32[:, j, :]

    def spread_b(core, xx):
        stg8[...] = gb[core, xx].astype(F32)
        for j in range(ROWS_B):
            wb[core * 4 + xx, :, j * LANES : (j + 1) * LANES] = stg8[:, j, :]

    spread_b(c, x)

    z_pair = at(z_=step(z, 4, NZ))
    load_late.wait()
    arrived(pr2.at[0 : NY - 1], "p1b")
    for yy in range(NY):
        pf2[4 * yy : 4 * yy + 4, :] = pr2[yy].astype(F32)
    q2[y, zh, x, c] = pf2[...].astype(BF16)
    load_early.wait()
    arrived(pr1.at[0 : NY - 1], "p1a")
    for yy in range(NY):
        pf1[4 * yy : 4 * yy + 4, :] = pr1[yy].astype(F32)
    q1[zh, x, c] = pf1[...].astype(BF16)

    arrived(ga.at[c, :, 0 : NZ - 1], "gaz")
    send(ga.at[c], ga.at[c], "gac", sibling)
    send(q2.at[y, zh, x, c], q2.at[y, zh, x, c], "p2b", z_pair)
    spread_a(c)
    arrived(gb.at[c, 0 : NX - 1], "gbx")
    for d in range(1, NX):
        send(gb.at[c, from_x[d]], gb.at[c, from_x[d]], "gbc", sibling)
        spread_b(c, from_x[d])
    for d in range(1, NX):
        send(q1.at[zh, x, c], q1.at[zh, x, c], "p3a", at(x_=xs[d]))
    arrived(ga.at[other], "gac")
    send(q1.at[zh, x, c], q1.at[zh, x, c], "p2a", z_pair)
    spread_a(other)
    arrived(gb.at[other], "gbc")
    for d in range(NX):
        spread_b(other, from_x[d])

    load_act.wait()
    load_cot.wait()
    for one in loads[2:]:
        one.wait()
    wide_a = wa[...].reshape(RANK, ROWS_A * LANES).astype(BF16)
    wide_b = wb[...].reshape(RANK, ROWS_B * LANES).astype(BF16)
    low[y, :, 0:RANK] = dot_nt(act[...], wide_a).astype(BF16)
    low[y, :, RANK : 2 * RANK] = dot_nt(cot[...], wide_b).astype(BF16)
    for d in range(1, NY):
        send(low.at[y], low.at[y], "low", at(y_=ys[d]))
    arrived(q2.at[y, 1 - zh, x, c], "p2b")
    for d in range(1, NX):
        send(q2.at[y, :, x, c], q2.at[y, :, x, c], "p3b", at(x_=xs[d]))
    drain("gax", "gaz", "gac", "gbz", "gbx", "gbc", "p1a", "p1b")
    arrived(low.at[0 : NY - 1], "low")
    total = low[0].astype(F32)
    for yy in range(1, NY):
        total = total + low[yy].astype(F32)
    kept = (total * keep_ref[0].astype(F32)).T.astype(BF16)
    input_kept, grad_kept = kept[0:RANK], kept[RANK : 2 * RANK]

    chunk = 4
    for first in range(0, ROWS_A, chunk):
        part = dot_nn(grad_kept, act[:, first * LANES : (first + chunk) * LANES])
        for j in range(chunk):
            sa[:, first + j, :] = part[:, j * LANES : (j + 1) * LANES]
    mine, theirs = pl.ds(c * 32, 32), pl.ds(other * 32, 32)
    pa[...] = sa[theirs].reshape(NX, NZ, ROWS_A, LANES).astype(BF16)
    send(pa, r1a, "c1a", sibling)
    for first in range(0, ROWS_B, chunk):
        part = dot_nn(input_kept, cot[:, first * LANES : (first + chunk) * LANES])
        for j in range(chunk):
            sb[:, first + j, :] = part[:, j * LANES : (j + 1) * LANES]

    order = [1, 2, 3, 0]
    for d in order:
        rows = pl.ds(other * 32 + xs[d] * 8, 8)
        pb[d] = sb[rows].astype(BF16)
        send(pb.at[d], r1b.at[d], f"c1b{d}", sibling)
    arrived(r1a, "c1a")
    pair_a = sa[mine].reshape(NX, NZ, ROWS_A, LANES) + r1a[...].astype(F32)
    f2a[...] = pair_a
    s2a[...] = pair_a.astype(BF16)
    for d in range(1, NZ):
        send(s2a.at[:, zs[d]], r2a.at[d], "c2a", at(z_=zs[d]))
    for d in order:
        arrived(r1b.at[d], f"c1b{d}")
        rows = pl.ds(c * 32 + xs[d] * 8, 8)
        pair = sb[rows] + r1b[d].astype(F32)
        if d:
            s2b[d] = pair.astype(BF16)
            send(s2b.at[d], r2b.at[d], "c2b", at(x_=xs[d]))
        else:
            t32b[...] = pair
    arrived(q2.at[y, :, 0 : NX - 1, c], "p3b")
    for d in range(1, NY):
        send(q2.at[y, :, :, c], q2.at[y, :, :, c], "p4b", at(y_=ys[d]))
    drain("low", "c1a", *(f"c1b{d}" for d in order), "p2b")
    arrived(r2b.at[1:NX], "c2b")
    column = t32b[...]
    for d in range(1, NX):
        column = column + r2b[d].astype(F32)
    t32b[...] = column
    t16b[...] = column.astype(BF16)
    for d in range(1, NZ):
        send(t16b.at[zs[d]], r3b.at[d], "c3b", at(z_=zs[d]))
    arrived(r2a.at[1:NZ], "c2a")
    line = f2a[:, z]
    for d in range(1, NZ):
        line = line + r2a[d].astype(F32)
    t32a[...] = line
    t16a[...] = line.astype(BF16)
    for d in range(1, NX):
        send(t16a.at[xs[d]], r3a.at[d], "c3a", at(x_=xs[d]))
    arrived(q1.at[1 - zh, x, c], "p2a")
    for d in range(1, NX):
        send(q1.at[1 - zh, x, c], q1.at[1 - zh, x, c], "p3c", at(x_=xs[d]))
    send(q2.at[y, :, :, c], q2.at[y, :, :, c], "p5b", sibling)
    send(q1.at[:, x, c], q1.at[:, x, c], "p5a", sibling)
    arrived(q1.at[0, 0 : NX - 1, c], "p3a")
    scale = adapter_scale / ROLLOUT_TOKENS
    arrived(r3a.at[1:NX], "c3a")
    grad_a = t32a[x]
    for d in range(1, NX):
        grad_a = grad_a + r3a[d].astype(F32)
    grad_a = grad_a * scale
    new_a, _, _ = adam_update(fa[:, 0, :], ma[:, 0, :], va[:, 0, :], grad_a)
    for h in range(2):
        ez[h, z] = new_a[8 * h : 8 * h + 8].astype(BF16)
    for d in range(1, NZ):
        send(ez.at[:, z], ez.at[:, z], "ez", at(z_=zs[d]))
    arrived(r3b.at[1:NZ], "c3b")
    grad_b = t32b[z]
    for d in range(1, NZ):
        grad_b = grad_b + r3b[d].astype(F32)
    grad_b = grad_b * scale
    grad_out[0:ROWS_A] = grad_a
    grad_out[ROWS_A:ROWS] = grad_b
    new_b, _, _ = adam_update(fb[:, 0, :], mb[:, 0, :], vb[:, 0, :], grad_b)
    blocks = jnp.concatenate(in_wide_blocks(new_b), axis=0).astype(BF16)
    for kk in range(4):
        ebz[z, kk] = blocks[8 * kk : 8 * kk + 8]
    y_zh, y_x = lax.div(y, 2), lax.rem(y, 2)
    on_way = zh == y_zh
    holder = zh * 2 + lax.div(x, 2)
    holds = y == holder

    def arrived_if(condition, dst, stage):
        pl.when(condition)(lambda: arrived(dst, stage))

    for d in range(1, NZ):
        send_if(lax.div(zs[d], 4) == y_zh, ebz.at[z], ebz.at[z], "bz", d, at(z_=zs[d]))

    drain("c2a", "c2b", "c3a", "c3b", "p2a", "p3a", "p3b")
    arrived(ez.at[:, 0 : NZ - 1], "ez")
    for d in range(1, NX):
        send(ez.at[0], ea0.at[x], "ex", at(x_=xs[d]))
    for d in range(1, NY):
        send(ez.at[1], ea1.at[y], "ey", at(y_=ys[d]))
    ea0[x] = ez[0]
    ea1[y] = ez[1]
    arrived_if(on_way, ebz.at[0 : NZ - 1], "bz")

    def two_blocks(xx):
        return ebz.at[:, pl.ds(lax.rem(xx, 2) * 2, 2)]

    for d in range(1, NX):
        target = jnp.logical_and(on_way, lax.div(xs[d], 2) == y_x)
        send_if(target, two_blocks(xs[d]), ebx.at[x], "bx", d, at(x_=xs[d]))

    arrived(q2.at[0 : NY - 1, :, :, c], "p4b")
    for d in range(1, NY):
        send(q2.at[from_y[d], :, :, c], q2.at[from_y[d], :, :, c], "p5b", sibling)
    arrived(q1.at[0, 0 : NX - 1, c], "p3c")
    for d in range(1, NX):
        send(q1.at[:, from_x[d], c], q1.at[:, from_x[d], c], "p5a", sibling)
    arrived(ea0.at[0 : NX - 1], "ex")
    for xx in range(NX):
        stga[xx * NZ : (xx + 1) * NZ] = ea0[xx].astype(F32)
    for j in range(8):
        ha0[y, c, :, j * LANES : (j + 1) * LANES] = stga[:, j, :].astype(BF16)
    for d in range(1, NY):
        send(ha0.at[y, c], ha0.at[y, c], "fy", at(y_=ys[d]))
    send(ha0.at[y, c], ha0.at[y, c], "fc", sibling)
    @pl.when(holds)
    def _():
        ebx[x] = ebz[:, pl.ds(lax.rem(x, 2) * 2, 2)]
        arrived(ebx.at[0 : NX - 1], "bx")

    send_if(holds, ebx.at[:, :, other], ebd, "bc", 0, sibling)

    arrived(ea1.at[0 : NY - 1], "ey")
    for yy in range(NY):
        stgy[yy] = ea1[yy].astype(F32)
    for yy in range(NY):
        for j in range(8):
            ha1[yy, c, x, :, j * LANES : (j + 1) * LANES] = stgy[yy, :, j, :].astype(BF16)
    for d in range(1, NX):
        send(ha1.at[:, c, x], ha1.at[:, c, x], "fx", at(x_=xs[d]))
    send(ha1.at[:, c, x], ha1.at[:, c, x], "fd", sibling)

    @pl.when(holds)
    def _():
        for xx in range(NX):
            stgb[c, xx * NZ : (xx + 1) * NZ] = ebx[xx, :, c].astype(F32)
        arrived(ebd, "bc")
        for xx in range(NX):
            stgb[other, xx * NZ : (xx + 1) * NZ] = ebd[xx].astype(F32)
        for yy in range(NY):
            for cc in range(NC):
                for h in range(2):
                    bs[yy, cc, :, h * LANES : (h + 1) * LANES] = stgb[
                        cc, :, 2 * yy + h, :
                    ].astype(BF16)
        bb[...] = bs[y]

    for d in range(1, NY):
        send_if(holds, bs.at[ys[d]], bb, "by", d, at(y_=ys[d]))

    load_base.wait()
    arrived(q2.at[:, :, :, other], "p5b")
    total = jnp.zeros((BLOCK, 256), F32)
    for yy in range(NY):
        columns = slice(HALF + yy * PART, HALF + (yy + 1) * PART)
        total = total + dot_nt(base[:, columns], q2[yy].reshape(256, PART))
    part_out[...] = total

    arrived(q1.at[:, :, other], "p5a")
    part_out[...] = part_out[...] + dot_nt(base[:, 0:HALF], q1[...].reshape(256, HALF))
    b_sends = [("bz", d) for d in range(1, NZ)] + [("bx", d) for d in range(1, NX)]
    drain("ez", "ex", "ey", "p3c", "p4b", "p5a", "p5b", *b_sends)
    arrived(ha0.at[0 : NY - 1, c], "fy")
    for d in range(1, NY):
        send(ha0.at[from_y[d], c], ha0.at[from_y[d], c], "fc", sibling)
    arrived(ha1.at[:, c, 0 : NX - 1], "fx")
    for d in range(1, NX):
        send(ha1.at[:, c, from_x[d]], ha1.at[:, c, from_x[d]], "fd", sibling)
    arrived(ha0.at[:, other], "fc")
    arrived(ha1.at[:, other], "fd")

    arrived_if(y != holder, bb, "by")
    drain(*leaving)


ARRIVALS, SENDS = 37, 26


def in_hbm(array):
    return pltpu.with_memory_space_constraint(array, pltpu.HBM)


def exchange(act, cot, keep, fa, ma, va, fb, mb, vb, prompts, base):
    hbm = pl.BlockSpec(memory_space=pltpu.HBM)
    vmem = pl.BlockSpec(memory_space=pltpu.VMEM)
    smem = pl.BlockSpec(memory_space=pltpu.SMEM)
    tokens = act.shape[0]
    sds = jax.ShapeDtypeStruct
    tile_a, tile_b = (ROWS_A, LANES), (ROWS_B, LANES)
    return pl.pallas_call(
        exchange_kernel,
        out_shape=(
            sds((ROWS, LANES), F32),
            sds((NY, NC, 32, 1024), BF16),
            sds((NY, NC, NX, 8, 1024), BF16),
            sds((NC, 32, WIDE), BF16),
            sds((BLOCK, 256), F32),
            sds((2, NX, NC, 16, HALF), BF16),
            sds((NY, 2, NX, NC, 16, PART), BF16),
            sds(base.shape, BF16),
        ),
        in_specs=[hbm, hbm, smem] + [hbm] * 8,
        out_specs=(vmem,) * 8,
        scratch_shapes=[
            pltpu.VMEM(act.shape, BF16),
            pltpu.VMEM(cot.shape, BF16),
            pltpu.VMEM(fa.shape, F32),
            pltpu.VMEM(fa.shape, F32),
            pltpu.VMEM(fa.shape, F32),
            pltpu.VMEM(fb.shape, F32),
            pltpu.VMEM(fb.shape, F32),
            pltpu.VMEM(fb.shape, F32),
            pltpu.VMEM((NC, NX, NZ, *tile_a), BF16),
            pltpu.VMEM((NC, NX, NZ, *tile_b), BF16),
            pltpu.VMEM((32, *tile_a), F32),
            pltpu.VMEM((NZ, *tile_b), F32),
            pltpu.VMEM((NC, 32, ROWS_A * LANES), F32),
            pltpu.VMEM((NC * NX, NZ, ROWS_B * LANES), F32),
            pltpu.VMEM((NY, tokens, 2 * RANK), BF16),
            pltpu.VMEM((RANK, *tile_a), F32),
            pltpu.VMEM((RANK, *tile_b), F32),
            pltpu.VMEM((NX, NZ, *tile_a), BF16),
            pltpu.VMEM((NX, NZ, *tile_b), BF16),
            pltpu.VMEM((NX, NZ, *tile_a), BF16),
            pltpu.VMEM((NX, NZ, *tile_b), BF16),
            pltpu.VMEM((NX, NZ, *tile_a), F32),
            pltpu.VMEM((NX, NZ, *tile_a), BF16),
            pltpu.VMEM((NX, NZ, *tile_b), BF16),
            pltpu.VMEM((NZ, NX, *tile_a), BF16),
            pltpu.VMEM((NX, NZ, *tile_b), BF16),
            pltpu.VMEM((NX, *tile_a), F32),
            pltpu.VMEM((NZ, *tile_b), F32),
            pltpu.VMEM((NX, *tile_a), BF16),
            pltpu.VMEM((NZ, *tile_b), BF16),
            pltpu.VMEM((NX, *tile_a), BF16),
            pltpu.VMEM((NZ, *tile_b), BF16),
            pltpu.VMEM((2, NZ, 8, LANES), BF16),
            pltpu.VMEM((NX, NZ, 8, LANES), BF16),
            pltpu.VMEM((NY, NZ, 8, LANES), BF16),
            pltpu.VMEM((NX * NZ, 8, LANES), F32),
            pltpu.VMEM((NY, NZ, 8, LANES), F32),
            pltpu.VMEM((NZ, 4, 8, LANES), BF16),
            pltpu.VMEM((NX, NZ, 2, 8, LANES), BF16),
            pltpu.VMEM((NX, NZ, 8, LANES), BF16),
            pltpu.VMEM((NC, NX * NZ, 8, LANES), F32),
            pltpu.VMEM((NY, NC, 32, WIDE), BF16),
            pltpu.VMEM((NY, 4, 4096), BF16),
            pltpu.VMEM((NY, 4, 1024), BF16),
            pltpu.VMEM((16, 4096), F32),
            pltpu.VMEM((16, 1024), F32),
            pltpu.SemaphoreType.DMA((11,)),
            pltpu.SemaphoreType.DMA((SENDS,)),
            pltpu.SemaphoreType.DMA((ARRIVALS,)),
        ],
        compiler_params=pltpu.CompilerParams(
            collective_id=0, has_side_effects=True, vmem_limit_bytes=24 * 1024 * 1024
        ),
        cost_estimate=pl.CostEstimate(
            flops=200_000_000_000, bytes_accessed=8_000_000, transcendentals=0
        ),
        name="exchange",
    )(
        in_hbm(act),
        in_hbm(cot),
        keep,
        *map(in_hbm, (fa, ma, va, fb, mb, vb)),
        in_hbm(prompts),
        in_hbm(base),
    )


def merge_kernel(
    base,
    ha0,
    ha1,
    bb,
    part,
    q1,
    q2,
    grad,
    fa,
    ma,
    va,
    fb,
    mb,
    vb,
    ua,
    ub,
    na,
    nb,
    sa,
    sb,
    merged,
    proj,
    rows,
    done,
):
    turned = (adapter_scale * bb[...].reshape(RANK, WIDE).astype(F32).T).astype(BF16)[0:BLOCK]
    cross = jnp.zeros((256, RANK), F32)
    copies = []
    for yy in range(NY):
        left = ha0[yy].reshape(RANK, PART)
        right = ha1[yy].astype(F32).reshape(RANK, PART).astype(BF16)
        for h, columns in enumerate((left, right)):
            first = (2 * yy + h) * PART
            here = slice(first, first + PART)
            delta = dot_nn(turned, columns)
            rows[:, here] = (base[:, here].astype(F32) + delta).astype(BF16)
            one = pltpu.make_async_copy(rows.at[:, here], merged.at[:, here], done.at[2 * yy + h])
            one.start()
            copies.append(one)
            if yy < 2:
                asked = q1[:, :, :, :, first : first + PART]
            else:
                asked = q2[2 * (yy - 2) + h]
            cross = cross + dot_nt(asked.reshape(256, PART), columns)
    ua[:, 0, :], na[:, 0, :], sa[:, 0, :] = adam_update(
        fa[:, 0, :], ma[:, 0, :], va[:, 0, :], grad[0:ROWS_A]
    )
    ub[:, 0, :], nb[:, 0, :], sb[:, 0, :] = adam_update(
        fb[:, 0, :], mb[:, 0, :], vb[:, 0, :], grad[ROWS_A:ROWS]
    )
    high = cross.astype(BF16)
    rest = (cross - high.astype(F32)).astype(BF16)
    proj[...] = (part[...] + dot_nt(turned, high) + dot_nt(turned, rest)).astype(BF16)
    for one in copies:
        one.wait()


def merge(base, ha0, ha1, bb, part, q1, q2, grad, fa, ma, va, fb, mb, vb):
    sds = jax.ShapeDtypeStruct
    vmem = pl.BlockSpec(memory_space=pltpu.VMEM)
    a_shape, b_shape = (ROWS_A, 1, LANES), (ROWS_B, 1, LANES)
    return pl.pallas_call(
        merge_kernel,
        out_shape=(
            sds(a_shape, F32),
            sds(b_shape, F32),
            sds(a_shape, F32),
            sds(b_shape, F32),
            sds(a_shape, F32),
            sds(b_shape, F32),
            sds(base.shape, BF16),
            sds((BLOCK, 256), BF16),
        ),
        in_specs=[vmem] * 14,
        out_specs=(vmem,) * 6 + (pl.BlockSpec(memory_space=pltpu.HBM), vmem),
        scratch_shapes=[pltpu.VMEM(base.shape, BF16), pltpu.SemaphoreType.DMA((2 * NY,))],
        compiler_params=pltpu.CompilerParams(vmem_limit_bytes=16 * 1024 * 1024),
        name="merge",
    )(base, ha0, ha1, bb, part, q1, q2, grad, fa, ma, va, fb, mb, vb)


def body(
    activations,
    cotangent,
    block_keep,
    input_factor,
    input_mean,
    input_square,
    output_factor,
    output_mean,
    output_square,
    frozen_base_rows,
    prompts,
):
    fa, ma, va = (v.reshape(ROWS_A, 1, LANES) for v in (input_factor, input_mean, input_square))
    fb, mb, vb = (v.reshape(ROWS_B, 1, LANES) for v in (output_factor, output_mean, output_square))
    grad, ha0, ha1, bb, part, q1, q2, base = exchange(
        activations,
        cotangent,
        block_keep,
        fa,
        ma,
        va,
        fb,
        mb,
        vb,
        prompts,
        frozen_base_rows,
    )
    ua, ub, na, nb, sa, sb, merged, projected = merge(
        base, ha0, ha1, bb, part, q1, q2, grad, fa, ma, va, fb, mb, vb
    )
    return (
        ua.reshape(1, -1),
        ub.reshape(1, -1),
        na.reshape(1, -1),
        nb.reshape(1, -1),
        sa.reshape(1, -1),
        sb.reshape(1, -1),
        merged,
        projected,
    )


def solution(mesh):
    row = P(("role", "dp"), "tp")
    placed = (
        row,
        row,
        P(("role", "dp")),
        row,
        row,
        row,
        row,
        row,
        row,
        P(("dp", "tp"), None),
        P(("role", "dp", "tp"), None),
    )
    return jax.shard_map(
        body,
        mesh=mesh,
        in_specs=placed,
        out_specs=(
            row,
            row,
            row,
            row,
            row,
            row,
            P(("dp", "tp"), None),
            P(("dp", "tp"), "role"),
        ),
        check_vma=False,
    )
```

```python
import jax
import jax.numpy as jnp
from jax import lax
from jax.experimental import pallas as pl
from jax.experimental.pallas import tpu as pltpu
from jax.sharding import PartitionSpec as P

ROLLOUT_TOKENS = 256
RANK = 64
LANES = 128
ROWS_A, ROWS_B = 16, 28
ROWS = ROWS_A + ROWS_B
NX, NY, NZ, NC = 4, 4, 8, 2
BLOCK = 224
WIDE = 256
HALF, PART = 4096, 1024

adapter_scale = 2.0
learn_rate = 0.004
beta_one = 0.9
beta_two = 0.95
epsilon = 1e-08
first_fix = 1.0 - 0.9**20
second_fix = 1.0 - 0.95**20

F32, BF16 = jnp.float32, jnp.bfloat16
MESH = pl.DeviceIdType.MESH


def adam_update(factor, moment, square, gradient):
    moment_new = beta_one * moment + (1.0 - beta_one) * gradient
    square_new = beta_two * square + (1.0 - beta_two) * gradient * gradient
    factor_new = factor - learn_rate * (moment_new / first_fix) / (
        jnp.sqrt(square_new / second_fix) + epsilon
    )
    return (factor_new, moment_new, square_new)


def dot_nn(a, b):
    return lax.dot_general(a, b, (((1,), (0,)), ((), ())), preferred_element_type=F32)


def dot_nt(a, b):
    return lax.dot_general(a, b, (((1,), (1,)), ((), ())), preferred_element_type=F32)


def in_wide_blocks(rows):
    lane = lax.broadcasted_iota(jnp.int32, (1, LANES), 1)
    rolled = {0: rows}
    for off in (32, 64, 96):
        rolled[off] = pltpu.roll(rows, LANES - off, 1)
    out = []
    for k in range(16):
        row, off = divmod(BLOCK * k, LANES)
        turned = rolled[off]
        for half in range(2):
            first = turned[row + half : row + half + 1]
            if off == 0:
                out.append(first)
                continue
            last = min(row + half + 1, ROWS_B - 1)
            second = turned[last : last + 1]
            out.append(jnp.where(lane < LANES - off, first, second))
    return out


def exchange_kernel(
    act_hbm,
    cot_hbm,
    keep_ref,
    fa_hbm,
    ma_hbm,
    va_hbm,
    fb_hbm,
    mb_hbm,
    vb_hbm,
    prompts_hbm,
    base_hbm,
    grad_out,
    ha0,
    ha1,
    bb,
    part_out,
    q1,
    q2,
    base,
    act,
    cot,
    fa,
    ma,
    va,
    fb,
    mb,
    vb,
    ga,
    gb,
    stg32,
    stg8,
    wa,
    wb,
    low,
    sa,
    sb,
    pa,
    pb,
    r1a,
    r1b,
    f2a,
    s2a,
    s2b,
    r2a,
    r2b,
    t32a,
    t32b,
    t16a,
    t16b,
    r3a,
    r3b,
    ez,
    ea0,
    ea1,
    stga,
    stgy,
    ebz,
    ebx,
    ebd,
    stgb,
    bs,
    pr1,
    pr2,
    pf1,
    pf2,
    loc,
    ssem,
    rsem,
):
    z_lo = lax.axis_index("role")
    dp = lax.axis_index("dp")
    y = lax.axis_index("tp")
    c = lax.rem(dp, 2)
    x = lax.rem(lax.div(dp, 2), 4)
    zh = lax.div(dp, 8)
    z = zh * 4 + z_lo

    def at(x_=x, y_=y, z_=z, c_=c):
        return {
            "role": lax.rem(z_, 4),
            "dp": lax.div(z_, 4) * 8 + x_ * 2 + c_,
            "tp": y_,
        }

    def step(v, d, n):
        return lax.rem(v + d, n)

    other = 1 - c
    sibling = at(c_=other)
    xs = [step(x, d, NX) for d in range(NX)]
    ys = [step(y, d, NY) for d in range(NY)]
    zs = [step(z, d, NZ) for d in range(NZ)]
    from_x = [step(x, NX - d, NX) for d in range(NX)]
    from_y = [step(y, NY - d, NY) for d in range(NY)]
    from_z = [step(z, NZ - d, NZ) for d in range(NZ)]

    stages, free, leaving, whole = {}, list(range(SENDS))[::-1], {}, {}

    def copy(src, dst, stage, key, device):
        return pltpu.make_async_remote_copy(
            src_ref=src,
            dst_ref=dst,
            send_sem=ssem.at[leaving[key][0]],
            recv_sem=rsem.at[stages.setdefault(stage, len(stages))],
            device_id=device,
            device_id_type=MESH,
        )

    def send(src, dst, stage, device):
        if stage not in leaving:
            leaving[stage] = (free.pop(), None, None)
        copy(src, dst, stage, stage, device).start()

    def send_if(condition, src, dst, stage, d, device):
        index = free.pop()
        leaving[stage, d] = (index, None, None)
        one = copy(src, dst, stage, (stage, d), device)
        leaving[stage, d] = (index, condition, one)
        pl.when(condition)(one.start)

    def arrived(all_of_it, stage):
        whole[stage] = all_of_it
        semaphore = rsem.at[stages[stage]]
        pltpu.make_async_copy(all_of_it, all_of_it, semaphore).wait()

    def drain(*keys):
        for key in keys:
            index, condition, one = leaving.pop(key)
            if one is None:
                pltpu.make_async_copy(whole[key], whole[key], ssem.at[index]).wait()
            else:
                pl.when(condition)(one.wait_send)
            free.append(index)

    load_act = pltpu.make_async_copy(act_hbm, act, loc.at[0])
    load_cot = pltpu.make_async_copy(cot_hbm, cot, loc.at[1])
    loads = [
        pltpu.make_async_copy(src, dst, loc.at[3 + i])
        for i, (src, dst) in enumerate(
            ((fa_hbm, fa), (fb_hbm, fb), (ma_hbm, ma), (va_hbm, va), (mb_hbm, mb), (vb_hbm, vb))
        )
    ]
    for one in loads[:2]:
        one.start()

    def late(yy):
        return prompts_hbm.at[:, pl.ds(pl.multiple_of(HALF + yy * PART, PART), PART)]

    early = prompts_hbm.at[:, 0:HALF]
    load_early = pltpu.make_async_copy(early, pr1.at[y], loc.at[2])
    load_late = pltpu.make_async_copy(late(y), pr2.at[y], loc.at[9])
    load_base = pltpu.make_async_copy(base_hbm, base, loc.at[10])
    load_early.start()
    load_late.start()
    load_act.start()
    load_cot.start()
    for one in loads[2:]:
        one.start()
    load_base.start()

    barrier = pltpu.get_barrier_semaphore()
    peers = (
        [sibling]
        + [at(x_=v) for v in xs[1:]]
        + [at(y_=v) for v in ys[1:]]
        + [at(z_=v) for v in zs[1:]]
    )
    for peer in peers:
        pl.semaphore_signal(barrier, inc=1, device_id=peer, device_id_type=MESH)

    for one in loads[:2]:
        one.wait()
    ga[c, x, z] = fa[:, 0, :].astype(BF16)
    gb[c, x, z] = fb[:, 0, :].astype(BF16)
    pl.semaphore_wait(barrier, len(peers))

    for d in range(1, NX):
        send(ga.at[c, x, z], ga.at[c, x, z], "gax", at(x_=xs[d]))
    for d in range(1, NZ):
        send(gb.at[c, x, z], gb.at[c, x, z], "gbz", at(z_=zs[d]))
    for d in range(1, NY):
        send(late(ys[d]), pr2.at[y], "p1b", at(y_=ys[d]))
    for d in range(1, NY):
        send(early, pr1.at[y], "p1a", at(y_=ys[d]))
    arrived(ga.at[c, 0 : NX - 1, z], "gax")
    for d in range(1, NZ):
        send(ga.at[c, :, z], ga.at[c, :, z], "gaz", at(z_=zs[d]))
    arrived(gb.at[c, x, 0 : NZ - 1], "gbz")
    for d in range(1, NX):
        send(gb.at[c, x], gb.at[c, x], "gbx", at(x_=xs[d]))
    send(gb.at[c, x], gb.at[c, x], "gbc0", sibling)

    def spread_a(core):
        stg32[...] = ga[core].reshape(32, ROWS_A, LANES).astype(F32)
        for j in range(ROWS_A):
            wa[core, :, j * LANES : (j + 1) * LANES] = stg32[:, j, :]

    def spread_b(core, xx):
        stg8[...] = gb[core, xx].astype(F32)
        for j in range(ROWS_B):
            wb[core * 4 + xx, :, j * LANES : (j + 1) * LANES] = stg8[:, j, :]

    spread_b(c, x)

    z_pair = at(z_=step(z, 4, NZ))
    load_late.wait()
    arrived(pr2.at[0 : NY - 1], "p1b")
    for yy in range(NY):
        pf2[4 * yy : 4 * yy + 4, :] = pr2[yy].astype(F32)
    q2[y, zh, x, c] = pf2[...].astype(BF16)
    load_early.wait()
    arrived(pr1.at[0 : NY - 1], "p1a")
    for yy in range(NY):
        pf1[4 * yy : 4 * yy + 4, :] = pr1[yy].astype(F32)
    q1[zh, x, c] = pf1[...].astype(BF16)

    arrived(ga.at[c, :, 0 : NZ - 1], "gaz")
    send(ga.at[c], ga.at[c], "gac", sibling)
    send(q2.at[y, zh, x, c], q2.at[y, zh, x, c], "p2b", z_pair)
    spread_a(c)
    arrived(gb.at[c, 0 : NX - 1], "gbx")
    for d in range(1, NX):
        send(gb.at[c, from_x[d]], gb.at[c, from_x[d]], f"gbc{d}", sibling)
        spread_b(c, from_x[d])
    for d in range(1, NX):
        send(q1.at[zh, x, c], q1.at[zh, x, c], "p3a", at(x_=xs[d]))
    arrived(ga.at[other], "gac")
    send(q1.at[zh, x, c], q1.at[zh, x, c], "p2a", z_pair)
    spread_a(other)
    for d in range(NX):
        arrived(gb.at[other, from_x[d]], f"gbc{d}")
        spread_b(other, from_x[d])

    load_act.wait()
    load_cot.wait()
    for one in loads[2:]:
        one.wait()
    wide_a = wa[...].reshape(RANK, ROWS_A * LANES).astype(BF16)
    wide_b = wb[...].reshape(RANK, ROWS_B * LANES).astype(BF16)
    low[y, :, 0:RANK] = dot_nt(act[...], wide_a).astype(BF16)
    low[y, :, RANK : 2 * RANK] = dot_nt(cot[...], wide_b).astype(BF16)
    for d in range(1, NY):
        send(low.at[y], low.at[y], "low", at(y_=ys[d]))
    arrived(q2.at[y, 1 - zh, x, c], "p2b")
    for d in range(1, NX):
        send(q2.at[y, :, x, c], q2.at[y, :, x, c], "p3b", at(x_=xs[d]))
    drain("gax", "gaz", "gac", "gbz", "gbx", *(f"gbc{d}" for d in range(NX)), "p1a", "p1b")
    arrived(low.at[0 : NY - 1], "low")
    total = low[0].astype(F32)
    for yy in range(1, NY):
        total = total + low[yy].astype(F32)
    kept = (total * keep_ref[0].astype(F32)).T.astype(BF16)
    input_kept, grad_kept = kept[0:RANK], kept[RANK : 2 * RANK]

    chunk = 4
    for first in range(0, ROWS_A, chunk):
        part = dot_nn(grad_kept, act[:, first * LANES : (first + chunk) * LANES])
        for j in range(chunk):
            sa[:, first + j, :] = part[:, j * LANES : (j + 1) * LANES]
    mine, theirs = pl.ds(c * 32, 32), pl.ds(other * 32, 32)
    pa[...] = sa[theirs].reshape(NX, NZ, ROWS_A, LANES).astype(BF16)
    send(pa, r1a, "c1a", sibling)
    for first in range(0, ROWS_B, chunk):
        part = dot_nn(input_kept, cot[:, first * LANES : (first + chunk) * LANES])
        for j in range(chunk):
            sb[:, first + j, :] = part[:, j * LANES : (j + 1) * LANES]

    order = [1, 2, 3, 0]
    for d in order:
        rows = pl.ds(other * 32 + xs[d] * 8, 8)
        pb[d] = sb[rows].astype(BF16)
        send(pb.at[d], r1b.at[d], f"c1b{d}", sibling)
    arrived(r1a, "c1a")
    pair_a = sa[mine].reshape(NX, NZ, ROWS_A, LANES) + r1a[...].astype(F32)
    f2a[...] = pair_a
    s2a[...] = pair_a.astype(BF16)
    for d in range(1, NZ):
        send(s2a.at[:, zs[d]], r2a.at[d], "c2a", at(z_=zs[d]))
    for d in order:
        arrived(r1b.at[d], f"c1b{d}")
        rows = pl.ds(c * 32 + xs[d] * 8, 8)
        pair = sb[rows] + r1b[d].astype(F32)
        if d:
            s2b[d] = pair.astype(BF16)
            send(s2b.at[d], r2b.at[d], "c2b", at(x_=xs[d]))
        else:
            t32b[...] = pair
    arrived(q2.at[y, :, 0 : NX - 1, c], "p3b")
    for d in range(1, NY):
        send(q2.at[y, :, :, c], q2.at[y, :, :, c], "p4b", at(y_=ys[d]))
    drain("low", "c1a", *(f"c1b{d}" for d in order), "p2b")
    arrived(r2b.at[1:NX], "c2b")
    column = t32b[...]
    for d in range(1, NX):
        column = column + r2b[d].astype(F32)
    t32b[...] = column
    t16b[...] = column.astype(BF16)
    for d in range(1, NZ):
        send(t16b.at[zs[d]], r3b.at[d], "c3b", at(z_=zs[d]))
    arrived(r2a.at[1:NZ], "c2a")
    line = f2a[:, z]
    for d in range(1, NZ):
        line = line + r2a[d].astype(F32)
    t32a[...] = line
    t16a[...] = line.astype(BF16)
    for d in range(1, NX):
        send(t16a.at[xs[d]], r3a.at[d], "c3a", at(x_=xs[d]))
    arrived(q1.at[1 - zh, x, c], "p2a")
    for d in range(1, NX):
        send(q1.at[1 - zh, x, c], q1.at[1 - zh, x, c], "p3c", at(x_=xs[d]))
    send(q2.at[y, :, :, c], q2.at[y, :, :, c], "p5b", sibling)
    send(q1.at[:, x, c], q1.at[:, x, c], "p5a", sibling)
    arrived(q1.at[0, 0 : NX - 1, c], "p3a")
    scale = adapter_scale / ROLLOUT_TOKENS
    arrived(r3a.at[1:NX], "c3a")
    grad_a = t32a[x]
    for d in range(1, NX):
        grad_a = grad_a + r3a[d].astype(F32)
    grad_a = grad_a * scale
    new_a, _, _ = adam_update(fa[:, 0, :], ma[:, 0, :], va[:, 0, :], grad_a)
    for h in range(2):
        ez[h, z] = new_a[8 * h : 8 * h + 8].astype(BF16)
    for d in range(1, NZ):
        send(ez.at[:, z], ez.at[:, z], "ez", at(z_=zs[d]))
    arrived(r3b.at[1:NZ], "c3b")
    grad_b = t32b[z]
    for d in range(1, NZ):
        grad_b = grad_b + r3b[d].astype(F32)
    grad_b = grad_b * scale
    grad_out[0:ROWS_A] = grad_a
    grad_out[ROWS_A:ROWS] = grad_b
    new_b, _, _ = adam_update(fb[:, 0, :], mb[:, 0, :], vb[:, 0, :], grad_b)
    blocks = jnp.concatenate(in_wide_blocks(new_b), axis=0).astype(BF16)
    for kk in range(4):
        ebz[z, kk] = blocks[8 * kk : 8 * kk + 8]
    y_zh, y_x = lax.div(y, 2), lax.rem(y, 2)
    on_way = zh == y_zh
    holder = zh * 2 + lax.div(x, 2)
    holds = y == holder

    def arrived_if(condition, dst, stage):
        pl.when(condition)(lambda: arrived(dst, stage))

    for d in range(1, NZ):
        send_if(lax.div(zs[d], 4) == y_zh, ebz.at[z], ebz.at[z], "bz", d, at(z_=zs[d]))

    drain("c2a", "c2b", "c3a", "c3b", "p2a", "p3a", "p3b")
    arrived(ez.at[:, 0 : NZ - 1], "ez")
    for d in range(1, NX):
        send(ez.at[0], ea0.at[x], "ex", at(x_=xs[d]))
    for d in range(1, NY):
        send(ez.at[1], ea1.at[y], "ey", at(y_=ys[d]))
    ea0[x] = ez[0]
    ea1[y] = ez[1]
    arrived_if(on_way, ebz.at[0 : NZ - 1], "bz")

    def two_blocks(xx):
        return ebz.at[:, pl.ds(lax.rem(xx, 2) * 2, 2)]

    for d in range(1, NX):
        target = jnp.logical_and(on_way, lax.div(xs[d], 2) == y_x)
        send_if(target, two_blocks(xs[d]), ebx.at[x], "bx", d, at(x_=xs[d]))

    arrived(q2.at[0 : NY - 1, :, :, c], "p4b")
    for d in range(1, NY):
        send(q2.at[from_y[d], :, :, c], q2.at[from_y[d], :, :, c], "p5b", sibling)
    arrived(q1.at[0, 0 : NX - 1, c], "p3c")
    for d in range(1, NX):
        send(q1.at[:, from_x[d], c], q1.at[:, from_x[d], c], "p5a", sibling)
    load_base.wait()
    arrived(q2.at[:, :, :, other], "p5b")
    total = jnp.zeros((BLOCK, 256), F32)
    for yy in range(NY):
        columns = slice(HALF + yy * PART, HALF + (yy + 1) * PART)
        total = total + dot_nt(base[:, columns], q2[yy].reshape(256, PART))
    part_out[...] = total

    arrived(ea0.at[0 : NX - 1], "ex")
    for xx in range(NX):
        stga[xx * NZ : (xx + 1) * NZ] = ea0[xx].astype(F32)
    for j in range(8):
        ha0[y, c, :, j * LANES : (j + 1) * LANES] = stga[:, j, :].astype(BF16)
    for d in range(1, NY):
        send(ha0.at[y, c], ha0.at[y, c], "fy", at(y_=ys[d]))
    send(ha0.at[y, c], ha0.at[y, c], "fc", sibling)
    @pl.when(holds)
    def _():
        ebx[x] = ebz[:, pl.ds(lax.rem(x, 2) * 2, 2)]
        arrived(ebx.at[0 : NX - 1], "bx")

    send_if(holds, ebx.at[:, :, other], ebd, "bc", 0, sibling)

    arrived(ea1.at[0 : NY - 1], "ey")
    for yy in range(NY):
        stgy[yy] = ea1[yy].astype(F32)
    for yy in range(NY):
        for j in range(8):
            ha1[yy, c, x, :, j * LANES : (j + 1) * LANES] = stgy[yy, :, j, :].astype(BF16)
    for d in range(1, NX):
        send(ha1.at[:, c, x], ha1.at[:, c, x], "fx", at(x_=xs[d]))
    send(ha1.at[:, c, x], ha1.at[:, c, x], "fd", sibling)

    @pl.when(holds)
    def _():
        for xx in range(NX):
            stgb[c, xx * NZ : (xx + 1) * NZ] = ebx[xx, :, c].astype(F32)
        arrived(ebd, "bc")
        for xx in range(NX):
            stgb[other, xx * NZ : (xx + 1) * NZ] = ebd[xx].astype(F32)
        for yy in range(NY):
            for cc in range(NC):
                for h in range(2):
                    bs[yy, cc, :, h * LANES : (h + 1) * LANES] = stgb[
                        cc, :, 2 * yy + h, :
                    ].astype(BF16)
        bb[...] = bs[y]

    for d in range(1, NY):
        send_if(holds, bs.at[ys[d]], bb, "by", d, at(y_=ys[d]))

    arrived(q1.at[:, :, other], "p5a")
    part_out[...] = part_out[...] + dot_nt(base[:, 0:HALF], q1[...].reshape(256, HALF))
    b_sends = [("bz", d) for d in range(1, NZ)] + [("bx", d) for d in range(1, NX)]
    drain("ez", "ex", "ey", "p3c", "p4b", "p5a", "p5b", *b_sends)
    arrived(ha0.at[0 : NY - 1, c], "fy")
    for d in range(1, NY):
        send(ha0.at[from_y[d], c], ha0.at[from_y[d], c], "fc", sibling)
    arrived(ha1.at[:, c, 0 : NX - 1], "fx")
    for d in range(1, NX):
        send(ha1.at[:, c, from_x[d]], ha1.at[:, c, from_x[d]], "fd", sibling)
    arrived(ha0.at[:, other], "fc")
    arrived(ha1.at[:, other], "fd")

    arrived_if(y != holder, bb, "by")
    drain(*leaving)


ARRIVALS, SENDS = 40, 26


def in_hbm(array):
    return pltpu.with_memory_space_constraint(array, pltpu.HBM)


def exchange(act, cot, keep, fa, ma, va, fb, mb, vb, prompts, base):
    hbm = pl.BlockSpec(memory_space=pltpu.HBM)
    vmem = pl.BlockSpec(memory_space=pltpu.VMEM)
    smem = pl.BlockSpec(memory_space=pltpu.SMEM)
    tokens = act.shape[0]
    sds = jax.ShapeDtypeStruct
    tile_a, tile_b = (ROWS_A, LANES), (ROWS_B, LANES)
    return pl.pallas_call(
        exchange_kernel,
        out_shape=(
            sds((ROWS, LANES), F32),
            sds((NY, NC, 32, 1024), BF16),
            sds((NY, NC, NX, 8, 1024), BF16),
            sds((NC, 32, WIDE), BF16),
            sds((BLOCK, 256), F32),
            sds((2, NX, NC, 16, HALF), BF16),
            sds((NY, 2, NX, NC, 16, PART), BF16),
            sds(base.shape, BF16),
        ),
        in_specs=[hbm, hbm, smem] + [hbm] * 8,
        out_specs=(vmem,) * 8,
        scratch_shapes=[
            pltpu.VMEM(act.shape, BF16),
            pltpu.VMEM(cot.shape, BF16),
            pltpu.VMEM(fa.shape, F32),
            pltpu.VMEM(fa.shape, F32),
            pltpu.VMEM(fa.shape, F32),
            pltpu.VMEM(fb.shape, F32),
            pltpu.VMEM(fb.shape, F32),
            pltpu.VMEM(fb.shape, F32),
            pltpu.VMEM((NC, NX, NZ, *tile_a), BF16),
            pltpu.VMEM((NC, NX, NZ, *tile_b), BF16),
            pltpu.VMEM((32, *tile_a), F32),
            pltpu.VMEM((NZ, *tile_b), F32),
            pltpu.VMEM((NC, 32, ROWS_A * LANES), F32),
            pltpu.VMEM((NC * NX, NZ, ROWS_B * LANES), F32),
            pltpu.VMEM((NY, tokens, 2 * RANK), BF16),
            pltpu.VMEM((RANK, *tile_a), F32),
            pltpu.VMEM((RANK, *tile_b), F32),
            pltpu.VMEM((NX, NZ, *tile_a), BF16),
            pltpu.VMEM((NX, NZ, *tile_b), BF16),
            pltpu.VMEM((NX, NZ, *tile_a), BF16),
            pltpu.VMEM((NX, NZ, *tile_b), BF16),
            pltpu.VMEM((NX, NZ, *tile_a), F32),
            pltpu.VMEM((NX, NZ, *tile_a), BF16),
            pltpu.VMEM((NX, NZ, *tile_b), BF16),
            pltpu.VMEM((NZ, NX, *tile_a), BF16),
            pltpu.VMEM((NX, NZ, *tile_b), BF16),
            pltpu.VMEM((NX, *tile_a), F32),
            pltpu.VMEM((NZ, *tile_b), F32),
            pltpu.VMEM((NX, *tile_a), BF16),
            pltpu.VMEM((NZ, *tile_b), BF16),
            pltpu.VMEM((NX, *tile_a), BF16),
            pltpu.VMEM((NZ, *tile_b), BF16),
            pltpu.VMEM((2, NZ, 8, LANES), BF16),
            pltpu.VMEM((NX, NZ, 8, LANES), BF16),
            pltpu.VMEM((NY, NZ, 8, LANES), BF16),
            pltpu.VMEM((NX * NZ, 8, LANES), F32),
            pltpu.VMEM((NY, NZ, 8, LANES), F32),
            pltpu.VMEM((NZ, 4, 8, LANES), BF16),
            pltpu.VMEM((NX, NZ, 2, 8, LANES), BF16),
            pltpu.VMEM((NX, NZ, 8, LANES), BF16),
            pltpu.VMEM((NC, NX * NZ, 8, LANES), F32),
            pltpu.VMEM((NY, NC, 32, WIDE), BF16),
            pltpu.VMEM((NY, 4, 4096), BF16),
            pltpu.VMEM((NY, 4, 1024), BF16),
            pltpu.VMEM((16, 4096), F32),
            pltpu.VMEM((16, 1024), F32),
            pltpu.SemaphoreType.DMA((11,)),
            pltpu.SemaphoreType.DMA((SENDS,)),
            pltpu.SemaphoreType.DMA((ARRIVALS,)),
        ],
        compiler_params=pltpu.CompilerParams(
            collective_id=0, has_side_effects=True, vmem_limit_bytes=24 * 1024 * 1024
        ),
        cost_estimate=pl.CostEstimate(
            flops=200_000_000_000, bytes_accessed=8_000_000, transcendentals=0
        ),
        name="exchange",
    )(
        in_hbm(act),
        in_hbm(cot),
        keep,
        *map(in_hbm, (fa, ma, va, fb, mb, vb)),
        in_hbm(prompts),
        in_hbm(base),
    )


def merge_kernel(
    base,
    ha0,
    ha1,
    bb,
    part,
    q1,
    q2,
    grad,
    fa,
    ma,
    va,
    fb,
    mb,
    vb,
    ua,
    ub,
    na,
    nb,
    sa,
    sb,
    merged,
    proj,
    rows,
    done,
):
    turned = (adapter_scale * bb[...].reshape(RANK, WIDE).astype(F32).T).astype(BF16)[0:BLOCK]
    cross = jnp.zeros((256, RANK), F32)
    copies = []
    for yy in range(NY):
        left = ha0[yy].reshape(RANK, PART)
        right = ha1[yy].astype(F32).reshape(RANK, PART).astype(BF16)
        for h, columns in enumerate((left, right)):
            first = (2 * yy + h) * PART
            here = slice(first, first + PART)
            delta = dot_nn(turned, columns)
            rows[:, here] = (base[:, here].astype(F32) + delta).astype(BF16)
            one = pltpu.make_async_copy(rows.at[:, here], merged.at[:, here], done.at[2 * yy + h])
            one.start()
            copies.append(one)
            if yy < 2:
                asked = q1[:, :, :, :, first : first + PART]
            else:
                asked = q2[2 * (yy - 2) + h]
            cross = cross + dot_nt(asked.reshape(256, PART), columns)
    ua[:, 0, :], na[:, 0, :], sa[:, 0, :] = adam_update(
        fa[:, 0, :], ma[:, 0, :], va[:, 0, :], grad[0:ROWS_A]
    )
    ub[:, 0, :], nb[:, 0, :], sb[:, 0, :] = adam_update(
        fb[:, 0, :], mb[:, 0, :], vb[:, 0, :], grad[ROWS_A:ROWS]
    )
    high = cross.astype(BF16)
    rest = (cross - high.astype(F32)).astype(BF16)
    proj[...] = (part[...] + dot_nt(turned, high) + dot_nt(turned, rest)).astype(BF16)
    for one in copies:
        one.wait()


def merge(base, ha0, ha1, bb, part, q1, q2, grad, fa, ma, va, fb, mb, vb):
    sds = jax.ShapeDtypeStruct
    vmem = pl.BlockSpec(memory_space=pltpu.VMEM)
    a_shape, b_shape = (ROWS_A, 1, LANES), (ROWS_B, 1, LANES)
    return pl.pallas_call(
        merge_kernel,
        out_shape=(
            sds(a_shape, F32),
            sds(b_shape, F32),
            sds(a_shape, F32),
            sds(b_shape, F32),
            sds(a_shape, F32),
            sds(b_shape, F32),
            sds(base.shape, BF16),
            sds((BLOCK, 256), BF16),
        ),
        in_specs=[vmem] * 14,
        out_specs=(vmem,) * 6 + (pl.BlockSpec(memory_space=pltpu.HBM), vmem),
        scratch_shapes=[pltpu.VMEM(base.shape, BF16), pltpu.SemaphoreType.DMA((2 * NY,))],
        compiler_params=pltpu.CompilerParams(vmem_limit_bytes=16 * 1024 * 1024),
        name="merge",
    )(base, ha0, ha1, bb, part, q1, q2, grad, fa, ma, va, fb, mb, vb)


def body(
    activations,
    cotangent,
    block_keep,
    input_factor,
    input_mean,
    input_square,
    output_factor,
    output_mean,
    output_square,
    frozen_base_rows,
    prompts,
):
    fa, ma, va = (v.reshape(ROWS_A, 1, LANES) for v in (input_factor, input_mean, input_square))
    fb, mb, vb = (v.reshape(ROWS_B, 1, LANES) for v in (output_factor, output_mean, output_square))
    grad, ha0, ha1, bb, part, q1, q2, base = exchange(
        activations,
        cotangent,
        block_keep,
        fa,
        ma,
        va,
        fb,
        mb,
        vb,
        prompts,
        frozen_base_rows,
    )
    ua, ub, na, nb, sa, sb, merged, projected = merge(
        base, ha0, ha1, bb, part, q1, q2, grad, fa, ma, va, fb, mb, vb
    )
    return (
        ua.reshape(1, -1),
        ub.reshape(1, -1),
        na.reshape(1, -1),
        nb.reshape(1, -1),
        sa.reshape(1, -1),
        sb.reshape(1, -1),
        merged,
        projected,
    )


def solution(mesh):
    row = P(("role", "dp"), "tp")
    placed = (
        row,
        row,
        P(("role", "dp")),
        row,
        row,
        row,
        row,
        row,
        row,
        P(("dp", "tp"), None),
        P(("role", "dp", "tp"), None),
    )
    return jax.shard_map(
        body,
        mesh=mesh,
        in_specs=placed,
        out_specs=(
            row,
            row,
            row,
            row,
            row,
            row,
            P(("dp", "tp"), None),
            P(("dp", "tp"), "role"),
        ),
        check_vma=False,
    )
```
